128 devices in a mesh: section: 8 (over x, z_hi), tensor: 4 (over z_lo, core), dp: 4 (over y).
Axes of the slice: x: 4, y: 4, z: 4 (z_hi: 2, z_lo: 2; z = z_hi * 2 + z_lo), core: 2. Of those that a mesh axis runs over, the one named last changes fastest.
Arguments:
- tokens: bfloat16 [64, 4096], P(None, ('section', 'dp')), may hold values from -100 to 100
- attn_gain: float32 [4096], P(('section', 'dp')), may hold values from 0.1 to 1.9
- qkv_weight: bfloat16 [4096, 10240], P(('section', 'dp'), 'tensor'), may hold values from -0.09375 to 0.09375
- qkv_order: int32 [10], replicated, may hold values from 0 to 9, each once
- cache_keys: bfloat16 [64, 8, 4096, 128], P(('section', 'dp'), 'tensor'), may hold values from -1300 to 1300
- cache_values: bfloat16 [64, 8, 4096, 128], P(('section', 'dp'), 'tensor'), may hold values from -6 to 6
- cache_len: int32 [64], P(('section', 'dp')), may hold values from 2 to 4096, as said below
- out_weight: bfloat16 [8192, 4096], P('tensor', ('section', 'dp')), may hold values from -0.0625 to 0.0625
- ffn_gain: float32 [4096], P(('section', 'dp')), may hold values from 0.1 to 1.9
- gate_up: bfloat16 [2, 4096, 28672], P(None, ('section', 'dp'), 'tensor'), may hold values from -0.09375 to 0.09375
- down_weight: bfloat16 [28672, 4096], P('tensor', ('section', 'dp')), may hold values from -0.03125 to 0.03125
Outputs:
- layer_out: bfloat16 [64, 4096], P(None, ('section', 'dp'))
The draws below stay inside these ranges and needn't reach their ends.
Inputs may be any that keep to these rules, and one draw needn't show every extreme that they name: qkv_order is a permutation of 0 to 9, the same for every key-value group. `cache_len`: at least one sequence has all 4096 positions valid.
All inputs are finite; a program needn't handle non-finite values.
Results may differ from the reference program's by a relative error of at most 0.0065.
Values may be sent and summed in bfloat16 or wider, within the bound.
A program may use at most 64 MiB of HBM per device.

```python
import math
import jax
import jax.numpy as jnp
from jax import lax

D = 4096
HEADS = 64
KV_HEADS = 8
HD = 128
FF = 28672
LEN = 4096
GROUP = 10
B = 64


def draw_tokens(key, part):
    key_base, key_rows, key_cols = jax.random.split(key, 3)
    normal_part = jnp.clip(jax.random.normal(key_base, (B, D), jnp.float32), -4.0, 4.0)
    column_scale = 3.0 ** (jnp.arange(D, dtype=jnp.float32) / (D - 1))
    column_scale = column_scale * jnp.exp(jax.random.uniform(key_cols, (1, D), jnp.float32, -0.35, 0.35))
    row_scale = jnp.exp(jax.random.uniform(key_rows, (B, 1), jnp.float32, math.log(0.3), math.log(3.0)))
    return (normal_part * row_scale * column_scale).astype(jnp.bfloat16)


def draw_cache_keys(key, part):
    key_base = jax.random.fold_in(key, 0)
    base_keys = 2.5 * jnp.clip(jax.random.normal(key_base, (B, KV_HEADS, LEN, HD), jnp.float32), -6.0, 6.0)
    return base_keys.astype(jnp.bfloat16)


def draw_cache_len(key, part):
    lengths = jax.random.randint(key, (B,), 2, LEN + 1, dtype=jnp.int32)
    return lengths.at[0].set(LEN)


def shard_levels(own_key, extent, cuts, low, top_value):
    factor_of = 1.0
    for axis_at, parts in cuts:
        draws = jax.random.uniform(jax.random.fold_in(jax.random.fold_in(own_key, 6), axis_at), (parts,), jnp.float32, low / len(cuts), top_value / len(cuts))
        factor_of = factor_of * jnp.repeat(jnp.exp(draws), extent[axis_at] // parts).reshape((-1,) + (1,) * (len(extent) - 1 - axis_at))
    return factor_of


def gaussian(key, dims, scale, reach, shards=(), held_as=jnp.bfloat16):
    drawn = jax.random.normal(key, dims, jnp.float32) * scale
    if len(shards) > 0:
        drawn = shard_levels(key, dims, shards, -0.22, 0.18) * drawn
    return jnp.clip(drawn, min=-reach, max=reach).astype(held_as)


def setup_inputs(seed: int = 0) -> dict:
    seeds = jax.random.split(jax.random.key(seed), 12)
    tokens = draw_tokens(jax.random.fold_in(seeds[11], 71), 0)
    attn_gain = jnp.clip(1.0 + 0.18 * jax.random.normal(seeds[1], (D,), jnp.float32), 0.1, 1.9)
    qkv_weight = gaussian(seeds[2], (D, KV_HEADS * GROUP * HD), D ** -0.5, 0.09375, ((0, 32), (1, 4)))
    qkv_order = jax.random.permutation(seeds[3], GROUP).astype(jnp.int32)
    cache_keys = draw_cache_keys(jax.random.fold_in(seeds[11], 71), 0)
    cache_values = gaussian(seeds[5], (B, KV_HEADS, LEN, HD), 1.0, 6.0, ((0, 32), (1, 4)))
    cache_len = draw_cache_len(jax.random.fold_in(seeds[11], 71), 0)
    out_weight = gaussian(seeds[7], (HEADS * HD, D), (HEADS * HD) ** -0.5, 0.0625, ((0, 4), (1, 32)))
    ffn_gain = jnp.clip(1.0 + 0.18 * jax.random.normal(seeds[8], (D,), jnp.float32), 0.1, 1.9)
    gate_up = gaussian(seeds[9], (2, D, FF), D ** -0.5, 0.09375, ((1, 32), (2, 4)))
    down_weight = gaussian(seeds[10], (FF, D), FF ** -0.5, 0.03125, ((0, 4), (1, 32)))
    return dict(tokens=tokens, attn_gain=attn_gain, qkv_weight=qkv_weight, qkv_order=qkv_order, cache_keys=cache_keys, cache_values=cache_values, cache_len=cache_len, out_weight=out_weight, ffn_gain=ffn_gain, gate_up=gate_up, down_weight=down_weight)


def normalize(stream, gain_vec):
    wide = stream.astype(jnp.float32)
    meansq = lax.optimization_barrier(jnp.mean(wide * wide, axis=-1, keepdims=True))
    return (wide * lax.rsqrt(meansq + 1e-05) * gain_vec.astype(jnp.float32)).astype(jnp.bfloat16)

def rotate(vector, cosine, sine_part):
    half_dim = vector.shape[-1] // 2
    first_half = vector[..., :half_dim]
    second = vector[..., half_dim:]
    return jnp.concatenate([first_half * cosine - second * sine_part, second * cosine + first_half * sine_part], axis=-1)

def attend_one(packed):
    queries, new_key, new_value, key_cache, value_cache, length = packed
    inv_scale = 1.0 / jnp.sqrt(jnp.float32(HD))
    scores = jnp.einsum('gpd,gld->gpl', queries.astype(jnp.float32), key_cache.astype(jnp.float32)) * inv_scale
    own_score = jnp.einsum('gpd,gd->gp', queries.astype(jnp.float32), new_key.astype(jnp.float32)) * inv_scale
    valid_mask = jnp.arange(LEN, dtype=jnp.int32) < length
    masked = jnp.where(valid_mask[None, None, :], scores, -jnp.inf)
    peak = jnp.maximum(lax.optimization_barrier(jnp.max(masked, axis=-1)), own_score)
    weights = jnp.exp(masked - peak[..., None])
    own_weight = jnp.exp(own_score - peak)
    denom_sum = lax.optimization_barrier(jnp.sum(weights, axis=-1)) + own_weight
    probabilities = (weights / denom_sum[..., None]).astype(jnp.bfloat16)
    own_prob = (own_weight / denom_sum).astype(jnp.bfloat16)
    mixed_heads = jnp.einsum('gpl,gld->gpd', probabilities.astype(jnp.float32), value_cache.astype(jnp.float32))
    mixed_heads = mixed_heads + own_prob.astype(jnp.float32)[..., None] * new_value.astype(jnp.float32)[:, None, :]
    return mixed_heads.astype(jnp.bfloat16).reshape(-1)

def reference(tokens, attn_gain, qkv_weight, qkv_order, cache_keys, cache_values, cache_len, out_weight, ffn_gain, gate_up, down_weight):
    per_group = HEADS // KV_HEADS
    normed = normalize(tokens, attn_gain)
    joined_cols = jnp.dot(normed, qkv_weight, preferred_element_type=jnp.float32)
    blocks = joined_cols.reshape(B, KV_HEADS, GROUP, HD)
    onehot = (qkv_order[:, None] == jnp.arange(GROUP, dtype=jnp.int32)[None, :]).astype(jnp.float32)
    logical = jnp.einsum('bgjd,ji->bgid', blocks, onehot, precision=lax.Precision.HIGHEST)
    half_dim = HD // 2
    inv_freq = 500000.0 ** (-(2.0 * jnp.arange(half_dim, dtype=jnp.float32)) / HD)
    angles = cache_len.astype(jnp.float32)[:, None] * inv_freq[None, :]
    cosine = jnp.cos(angles)
    sine_part = jnp.sin(angles)
    queries = rotate(logical[:, :, :per_group], cosine[:, None, None, :], sine_part[:, None, None, :]).astype(jnp.bfloat16)
    new_key = rotate(logical[:, :, per_group], cosine[:, None, :], sine_part[:, None, :]).astype(jnp.bfloat16)
    new_value = logical[:, :, per_group + 1].astype(jnp.bfloat16)
    attended = lax.map(attend_one, (queries, new_key, new_value, cache_keys, cache_values, cache_len))
    projected = jnp.dot(attended, out_weight, preferred_element_type=jnp.float32)
    hidden_state = (tokens.astype(jnp.float32) + projected).astype(jnp.bfloat16)
    ffn_normed = normalize(hidden_state, ffn_gain)
    gate = jnp.dot(ffn_normed, gate_up[0], preferred_element_type=jnp.float32)
    upward = jnp.dot(ffn_normed, gate_up[1], preferred_element_type=jnp.float32)
    activated = (jax.nn.silu(gate) * upward).astype(jnp.bfloat16)
    lowered = jnp.dot(activated, down_weight, preferred_element_type=jnp.float32)
    return (hidden_state.astype(jnp.float32) + lowered).astype(jnp.bfloat16)
```

```python
import jax
import jax.numpy as jnp
from jax import lax
from jax.experimental import pallas as pl
from jax.experimental.pallas import tpu as pltpu
from jax.sharding import PartitionSpec as P

D = 4096
HEADS = 64
KV_HEADS = 8
HD = 128
FF = 28672
LEN = 4096
GROUP = 10
B = 64
RANKS = 32
TENSOR = 4
DP = 4
SEQS = B // RANKS
LOCAL_GROUPS = KV_HEADS // TENSOR
PER_GROUP = HEADS // KV_HEADS
COLS = D // RANKS
SLOT_ROWS = 24
LOCAL_HEADS = HEADS // TENSOR
UNITS = FF // TENSOR
ROW_BLOCKS = 4
COL_BLOCKS = RANKS // ROW_BLOCKS
ROWS_EACH = B // ROW_BLOCKS
UNITS_EACH = UNITS // COL_BLOCKS
MESH = pl.DeviceIdType.MESH
F32 = jnp.float32
BF16 = jnp.bfloat16


def layer_kernel(
    order_ref,
    len_ref,
    tables_hbm,
    tokens_hbm,
    gains_hbm,
    qkv_hbm,
    keys_hbm,
    values_hbm,
    outw_hbm,
    gate_up_hbm,
    down_hbm,
    out_ref,
    tables,
    tokens,
    gains,
    qkvw,
    keys,
    values,
    outw,
    gate_up,
    down,
    joined32,
    joined_out,
    joined_in,
    att_out,
    att_in,
    att32,
    proj1,
    proj2,
    sq_out,
    sq_in,
    gu_out,
    gu_in,
    act,
    load_sem,
    send_sem,
    recv_sem,
):
    section = lax.axis_index("section")
    dp = lax.axis_index("dp")
    tensor = lax.axis_index("tensor")
    rank = section * DP + dp

    def load(i, src, dst):
        return pltpu.make_async_copy(src, dst, load_sem.at[i])

    loads = [
        load(0, tokens_hbm, tokens),
        load(1, gains_hbm, gains),
        load(2, qkv_hbm, qkvw),
        load(3, tables_hbm, tables),
        load(4, keys_hbm, keys),
        load(5, values_hbm, values),
        load(6, outw_hbm, outw),
        load(7, gate_up_hbm, gate_up),
        load(8, down_hbm, down),
    ]
    for copy in loads:
        copy.start()

    def peer(k):
        other = lax.rem(rank + k, RANKS)
        return other, {"section": other // DP, "dp": lax.rem(other, DP)}

    def tensor_peer(k):
        return {"tensor": lax.rem(tensor + k, TENSOR)}

    barrier = pltpu.get_barrier_semaphore()

    def greet(k, carry):
        pl.semaphore_signal(barrier, inc=1, device_id=peer(k)[1], device_id_type=MESH)
        return carry

    lax.fori_loop(1, RANKS, greet, 0)
    for k in range(1, TENSOR):
        pl.semaphore_signal(barrier, inc=1, device_id=tensor_peer(k), device_id_type=MESH)

    loads[0].wait()
    loads[1].wait()
    wide = tokens[...].astype(F32)
    squares = jnp.sum(wide * wide, axis=1, keepdims=True)
    left = jnp.broadcast_to(squares, (B, HD))
    for i in range(3):
        part = left.astype(BF16).astype(F32)
        joined32[:, 20 + i, :] = part
        left = left - part
    joined32[:, 23, :] = jnp.zeros((B, HD), F32)
    scaled = (wide * gains[0:1, :]).astype(BF16)
    loads[2].wait()
    for j in range(LOCAL_GROUPS * GROUP // 2):
        product = jnp.dot(scaled, qkvw[:, j * 256 : j * 256 + 256], preferred_element_type=F32)
        joined32[:, 2 * j, :] = product[:, :HD]
        joined32[:, 2 * j + 1, :] = product[:, HD:]

    def pack(i, carry):
        rows = joined32[pl.ds(i * SEQS, SEQS)]
        joined_out[i] = rows.reshape(SEQS * SLOT_ROWS, HD).astype(BF16)
        return carry

    lax.fori_loop(0, RANKS, pack, 0)
    joined_in[rank] = joined_out[rank]

    pl.semaphore_wait(barrier, RANKS - 1 + TENSOR - 1)

    def remote(src, dst, i, device):
        return pltpu.make_async_remote_copy(
            src_ref=src,
            dst_ref=dst,
            send_sem=send_sem.at[i],
            recv_sem=recv_sem.at[i],
            device_id=device,
            device_id_type=MESH,
        )

    def send_joined(k, carry):
        other, device = peer(k)
        remote(joined_out.at[other], joined_in.at[rank], 0, device).start()
        return carry

    lax.fori_loop(1, RANKS, send_joined, 0)

    def wait_all(src, dst, i):
        whole = remote(src, dst, i, peer(1)[1])
        whole.wait_send()
        whole.wait_recv()

    rest = pl.ds(0, RANKS - 1)
    wait_all(joined_out.at[rest], joined_in.at[rest], 0)

    joined = joined_in[0].astype(F32)
    for i in range(1, RANKS):
        joined = joined + joined_in[i].astype(F32)

    loads[3].wait()
    loads[4].wait()
    loads[5].wait()
    inv_scale = HD**-0.5
    position = lax.broadcasted_iota(jnp.int32, (PER_GROUP, LEN), 1)
    logical_row = lax.broadcasted_iota(jnp.int32, (16, HD), 0)
    for b in range(SEQS):
        base = b * SLOT_ROWS
        total = joined[base + 20 : base + 21] + joined[base + 21 : base + 22] + joined[base + 22 : base + 23]
        factor = lax.rsqrt(total / D + 1e-05)
        for g in range(LOCAL_GROUPS):
            logical = jnp.zeros((16, HD), F32)
            for j in range(GROUP):
                row = joined[base + g * GROUP + j : base + g * GROUP + j + 1]
                logical = jnp.where(logical_row == order_ref[j], row, logical)
            logical = logical * factor
            rotated = logical * tables[b : b + 1] + pltpu.roll(logical, HD // 2, 1) * tables[SEQS + b : SEQS + b + 1]
            rotated = rotated.astype(BF16)
            queries = rotated[0:PER_GROUP]
            new_key = rotated.astype(F32)[PER_GROUP : PER_GROUP + 1]
            new_value = logical[PER_GROUP + 1 : PER_GROUP + 2].astype(BF16).astype(F32)
            own = jnp.sum(queries.astype(F32) * new_key, axis=1, keepdims=True)
            scores = lax.dot_general(
                queries, keys[b, g], (((1,), (1,)), ((), ())), preferred_element_type=F32
            )
            masked = jnp.where(position < len_ref[b], scores, -jnp.inf)
            peak = jnp.maximum(jnp.max(masked, axis=1, keepdims=True), own)
            weights = jnp.exp((masked - peak) * inv_scale)
            own_weight = jnp.exp((own - peak) * inv_scale)
            denom = jnp.sum(weights, axis=1, keepdims=True) + own_weight
            mixed = jnp.dot(weights.astype(BF16), values[b, g], preferred_element_type=F32)
            mixed = mixed + own_weight.astype(BF16).astype(F32) * new_value
            att_out[pl.ds((b * LOCAL_GROUPS + g) * PER_GROUP, PER_GROUP)] = mixed / denom

    att_in[rank] = att_out[...].astype(BF16)

    def send_attended(k, carry):
        other, device = peer(k)
        remote(att_in.at[rank], att_in.at[rank], 1, device).start()
        return carry

    lax.fori_loop(1, RANKS, send_attended, 0)
    wait_all(att_in.at[rest], att_in.at[rest], 1)

    def widen(i, carry):
        att32[pl.ds(i * SEQS, SEQS)] = att_in[i].astype(F32).reshape(SEQS, LOCAL_HEADS, HD)
        return carry

    lax.fori_loop(0, RANKS, widen, 0)
    loads[6].wait()
    attended = jnp.concatenate([att32[:, h, :].astype(BF16) for h in range(LOCAL_HEADS)], axis=1)
    partial = jnp.dot(attended, outw[...], preferred_element_type=F32)

    def sum_over_tensor(value, buffer, i):
        buffer[tensor] = value
        for k in range(1, TENSOR):
            remote(buffer.at[tensor], buffer.at[tensor], i, tensor_peer(k)).start()
        others = pl.ds(0, TENSOR - 1)
        whole = remote(buffer.at[others], buffer.at[others], i, tensor_peer(1))
        whole.wait_send()
        whole.wait_recv()
        return buffer[0] + buffer[1] + buffer[2] + buffer[3]

    projected = sum_over_tensor(partial, proj1, 2)
    hidden = (tokens[...].astype(F32) + projected).astype(BF16).astype(F32)

    squares = jnp.sum(hidden * hidden, axis=1, keepdims=True)
    row_of = lax.broadcasted_iota(jnp.int32, (B, HD), 0)
    lane_of = lax.broadcasted_iota(jnp.int32, (B, HD), 1)
    sq_out[...] = jnp.sum(jnp.where(row_of == lane_of, squares, 0.0), axis=0, keepdims=True)
    sq_in[rank] = sq_out[...]

    def send_squares(k, carry):
        other, device = peer(k)
        remote(sq_out, sq_in.at[rank], 3, device).start()
        return carry

    lax.fori_loop(1, RANKS, send_squares, 0)
    scaled = (hidden * gains[1:2, :]).astype(BF16)
    loads[7].wait()
    my_rows = rank // COL_BLOCKS
    my_units = lax.rem(rank, COL_BLOCKS)

    def block_of(a, c):
        rows = pl.ds(pl.multiple_of(a * ROWS_EACH, ROWS_EACH), ROWS_EACH)
        units = pl.ds(pl.multiple_of(c * UNITS_EACH, 128), UNITS_EACH)
        return rows, units

    def produce(i, carry):
        c = lax.rem(my_units + i, COL_BLOCKS)
        units = pl.ds(pl.multiple_of(c * UNITS_EACH, 128), UNITS_EACH)
        for half in range(2):
            product = jnp.dot(scaled, gate_up[half, :, units], preferred_element_type=F32)
            gu_out[half, :, units] = product.astype(BF16)

        def send_block(j, inner):
            a = lax.rem(my_rows + j, ROW_BLOCKS)
            other = a * COL_BLOCKS + c
            rows, _ = block_of(a, c)

            @pl.when(other != rank)
            def _():
                device = {"section": other // DP, "dp": lax.rem(other, DP)}
                remote(gu_out.at[:, rows, units], gu_in.at[rank], 4, device).start()

            return inner

        lax.fori_loop(0, ROW_BLOCKS, send_block, 0)
        return carry

    lax.fori_loop(0, COL_BLOCKS, produce, 0)
    rows, units = block_of(my_rows, my_units)
    gu_in[rank] = gu_out[:, rows, units]
    wait_all(sq_in.at[rest], sq_in.at[rest], 3)
    total = jnp.sum(sq_in[...], axis=0)
    mine = lax.broadcasted_iota(jnp.int32, (ROWS_EACH, HD), 0) + my_rows * ROWS_EACH
    lane_of = lax.broadcasted_iota(jnp.int32, (ROWS_EACH, HD), 1)
    total = jnp.sum(jnp.where(mine == lane_of, total, 0.0), axis=1, keepdims=True)
    factor = lax.rsqrt(total / D + 1e-05)
    wait_all(gu_in.at[rest], gu_in.at[rest], 4)
    for j in range(UNITS_EACH // 128):
        lanes = slice(j * 128, j * 128 + 128)

        def add(i, sums):
            return (
                sums[0] + gu_in[i, 0, :, lanes].astype(F32),
                sums[1] + gu_in[i, 1, :, lanes].astype(F32),
            )

        zero = jnp.zeros((ROWS_EACH, 128), F32)
        gate, up = lax.fori_loop(0, RANKS, add, (zero, zero), unroll=8)
        gate = gate * factor
        up = up * factor
        value = gate / (1.0 + jnp.exp(-gate)) * up
        act[rows, pl.ds(pl.multiple_of(my_units * UNITS_EACH + j * 128, 128), 128)] = value.astype(BF16)

    def send_activated(k, carry):
        other, device = peer(k)
        remote(act.at[rows, units], act.at[rows, units], 5, device).start()
        return carry

    lax.fori_loop(1, RANKS, send_activated, 0)
    whole = remote(gu_in.at[rest, 0], gu_in.at[rest, 0], 5, peer(1)[1])
    whole.wait_send()
    whole.wait_recv()
    loads[8].wait()
    partial = jnp.dot(act[...], down[...], preferred_element_type=F32)
    lowered = sum_over_tensor(partial, proj2, 6)
    out_ref[...] = (hidden + lowered).astype(BF16)


def body(
    tokens,
    attn_gain,
    qkv_weight,
    qkv_order,
    cache_keys,
    cache_values,
    cache_len,
    out_weight,
    ffn_gain,
    gate_up,
    down_weight,
):
    half_dim = HD // 2
    inv_freq = 500000.0 ** (-(2.0 * jnp.arange(half_dim, dtype=F32)) / HD)
    angles = cache_len.astype(F32)[:, None] * inv_freq[None, :]
    cosine = jnp.cos(angles)
    sine = jnp.sin(angles)
    tables = jnp.concatenate(
        [jnp.concatenate([cosine, cosine], axis=1), jnp.concatenate([-sine, sine], axis=1)], axis=0
    )
    gains = jnp.stack([attn_gain, ffn_gain])
    smem = pl.BlockSpec(memory_space=pltpu.SMEM)
    hbm = pl.BlockSpec(memory_space=pl.ANY)
    return pl.pallas_call(
        layer_kernel,
        out_shape=jax.ShapeDtypeStruct((B, COLS), BF16),
        in_specs=[smem, smem] + [hbm] * 9,
        out_specs=pl.BlockSpec(memory_space=pltpu.VMEM),
        scratch_shapes=[
            pltpu.VMEM((2 * SEQS, HD), F32),
            pltpu.VMEM((B, COLS), BF16),
            pltpu.VMEM((2, COLS), F32),
            pltpu.VMEM(qkv_weight.shape, BF16),
            pltpu.VMEM(cache_keys.shape, BF16),
            pltpu.VMEM(cache_values.shape, BF16),
            pltpu.VMEM(out_weight.shape, BF16),
            pltpu.VMEM(gate_up.shape, BF16),
            pltpu.VMEM(down_weight.shape, BF16),
            pltpu.VMEM((B, SLOT_ROWS, HD), F32),
            pltpu.VMEM((RANKS, SEQS * SLOT_ROWS, HD), BF16),
            pltpu.VMEM((RANKS, SEQS * SLOT_ROWS, HD), BF16),
            pltpu.VMEM((SEQS * LOCAL_HEADS, HD), F32),
            pltpu.VMEM((RANKS, SEQS * LOCAL_HEADS, HD), BF16),
            pltpu.VMEM((B, LOCAL_HEADS, HD), F32),
            pltpu.VMEM((TENSOR, B, COLS), F32),
            pltpu.VMEM((TENSOR, B, COLS), F32),
            pltpu.VMEM((1, 128), F32),
            pltpu.VMEM((RANKS, 1, 128), F32),
            pltpu.VMEM((2, B, UNITS), BF16),
            pltpu.VMEM((RANKS, 2, ROWS_EACH, UNITS_EACH), BF16),
            pltpu.VMEM((B, UNITS), BF16),
            pltpu.SemaphoreType.DMA((9,)),
            pltpu.SemaphoreType.DMA((7,)),
            pltpu.SemaphoreType.DMA((7,)),
        ],
        compiler_params=pltpu.CompilerParams(
            collective_id=0, has_side_effects=True, vmem_limit_bytes=60 * 2**20
        ),
        name="decoder_layer",
    )(
        qkv_order,
        cache_len,
        tables,
        tokens,
        gains,
        qkv_weight,
        cache_keys,
        cache_values,
        out_weight,
        gate_up,
        down_weight,
    )


def solution(mesh):
    rows = P(None, ("section", "dp"))
    return jax.shard_map(
        body,
        mesh=mesh,
        in_specs=(
            rows,
            P(("section", "dp")),
            P(("section", "dp"), "tensor"),
            P(),
            P(("section", "dp"), "tensor", None, None),
            P(("section", "dp"), "tensor", None, None),
            P(("section", "dp")),
            P("tensor", ("section", "dp")),
            P(("section", "dp")),
            P(None, ("section", "dp"), "tensor"),
            P("tensor", ("section", "dp")),
        ),
        out_specs=rows,
        check_vma=False,
    )
```

```python
import jax
import jax.numpy as jnp
import numpy as np
from jax import lax
from jax.experimental import pallas as pl
from jax.experimental.pallas import tpu as pltpu
from jax.sharding import PartitionSpec as P

D = 4096
HEADS = 64
KV_HEADS = 8
HD = 128
FF = 28672
LEN = 4096
GROUP = 10
B = 64
RANKS = 32
TENSOR = 4
DP = 4
SEQS = B // RANKS
LOCAL_GROUPS = KV_HEADS // TENSOR
PER_GROUP = HEADS // KV_HEADS
COLS = D // RANKS
SLOT_ROWS = 24
LOCAL_HEADS = HEADS // TENSOR
UNITS = FF // TENSOR
SECTIONS = 8
NX, NY, NZ = 4, 4, 2
ROWS_EACH = B // NY
UNITS_EACH = UNITS // SECTIONS
CHUNKS = (("x", 0, 2), ("y", 2, 2), ("z", 4, 1), ("x", 5, 1), ("y", 6, 1))
MESH = pl.DeviceIdType.MESH
F32 = jnp.float32
BF16 = jnp.bfloat16


def layer_kernel(
    order_hbm,
    len_hbm,
    freq_hbm,
    tokens_hbm,
    gain1_hbm,
    gain2_hbm,
    qkv_hbm,
    keys_hbm,
    values_hbm,
    outw_hbm,
    gate_up_hbm,
    down_hbm,
    out_ref,
    order_ref,
    len_ref,
    freq,
    tokens,
    gains,
    qkvw,
    keys,
    values,
    outw,
    gate_up,
    down,
    joined32,
    joined_out,
    joined_in,
    att_out,
    att_in,
    att32,
    proj1,
    proj2,
    sq_out,
    sq_in,
    *rest_refs,
):
    gu_out, gu_in1, gu_sum, gu_in2, act = (rest_refs[5 * i : 5 * i + 5] for i in range(5))
    load_sem, send_sem, recv_sem = rest_refs[25:]
    section = lax.axis_index("section")
    x = section // NZ
    z = lax.rem(section, NZ)
    dp = lax.axis_index("dp")
    tensor = lax.axis_index("tensor")
    rank = section * DP + dp

    def load(i, src, dst):
        return pltpu.make_async_copy(src, dst, load_sem.at[i])

    loads = [
        load(0, tokens_hbm, tokens),
        load(1, gain1_hbm, gains.at[0]),
        load(2, qkv_hbm, qkvw),
        load(3, freq_hbm, freq),
        load(4, keys_hbm, keys),
        load(5, values_hbm, values),
        load(6, outw_hbm, outw),
        load(7, gate_up_hbm, gate_up),
        load(8, down_hbm, down),
        load(9, gain2_hbm, gains.at[1]),
        load(10, order_hbm, order_ref),
        load(11, len_hbm, len_ref),
    ]
    for copy in loads:
        copy.start()

    def peer(k):
        other = lax.rem(rank + k, RANKS)
        return other, {"section": other // DP, "dp": lax.rem(other, DP)}

    def tensor_peer(k):
        return {"tensor": lax.rem(tensor + k, TENSOR)}

    barrier = pltpu.get_barrier_semaphore()

    def greet(k, carry):
        pl.semaphore_signal(barrier, inc=1, device_id=peer(k)[1], device_id_type=MESH)
        return carry

    lax.fori_loop(1, RANKS, greet, 0)
    for k in range(1, TENSOR):
        pl.semaphore_signal(barrier, inc=1, device_id=tensor_peer(k), device_id_type=MESH)

    loads[0].wait()
    loads[1].wait()
    wide = tokens[...].astype(F32)
    squares = jnp.sum(wide * wide, axis=1, keepdims=True)
    left = jnp.broadcast_to(squares, (B, HD))
    for i in range(3):
        part = left.astype(BF16).astype(F32)
        joined32[:, 20 + i, :] = part
        left = left - part
    joined32[:, 23, :] = jnp.zeros((B, HD), F32)
    scaled = (wide * gains[0]).astype(BF16)
    loads[2].wait()
    for j in range(LOCAL_GROUPS * GROUP // 2):
        product = jnp.dot(scaled, qkvw[:, j * 256 : j * 256 + 256], preferred_element_type=F32)
        joined32[:, 2 * j, :] = product[:, :HD]
        joined32[:, 2 * j + 1, :] = product[:, HD:]

    def pack(i, carry):
        rows = joined32[pl.ds(i * SEQS, SEQS)]
        joined_out[i] = rows.reshape(SEQS * SLOT_ROWS, HD).astype(BF16)
        return carry

    lax.fori_loop(0, RANKS, pack, 0)
    for i in (3, 9, 10, 11):
        loads[i].wait()
    low = lax.broadcasted_iota(jnp.int32, (1, HD), 1) < HD // 2
    cosines, sines = [], []
    for b in range(SEQS):
        angle = freq[...] * len_ref[b].astype(F32)
        cosines.append(jnp.cos(angle))
        sine = jnp.sin(angle)
        sines.append(jnp.where(low, -sine, sine))
    joined_in[rank] = joined_out[rank]

    pl.semaphore_wait(barrier, RANKS - 1 + TENSOR - 1)

    def remote(src, dst, i, device):
        return pltpu.make_async_remote_copy(
            src_ref=src,
            dst_ref=dst,
            send_sem=send_sem.at[i],
            recv_sem=recv_sem.at[i],
            device_id=device,
            device_id_type=MESH,
        )

    def send_joined(k, carry):
        other, device = peer(k)
        remote(joined_out.at[other], joined_in.at[rank], 0, device).start()
        return carry

    lax.fori_loop(1, RANKS, send_joined, 0)

    def wait_all(src, dst, i):
        whole = remote(src, dst, i, peer(1)[1])
        whole.wait_send()
        whole.wait_recv()

    rest = pl.ds(0, RANKS - 1)
    wait_all(joined_out.at[rest], joined_in.at[rest], 0)

    joined = joined_in[0].astype(F32)
    for i in range(1, RANKS):
        joined = joined + joined_in[i].astype(F32)

    loads[4].wait()
    loads[5].wait()
    inv_scale = HD**-0.5
    position = lax.broadcasted_iota(jnp.int32, (PER_GROUP, LEN), 1)
    logical_row = lax.broadcasted_iota(jnp.int32, (16, HD), 0)
    for b in range(SEQS):
        base = b * SLOT_ROWS
        total = joined[base + 20 : base + 21] + joined[base + 21 : base + 22] + joined[base + 22 : base + 23]
        factor = lax.rsqrt(total / D + 1e-05)
        for g in range(LOCAL_GROUPS):
            logical = jnp.zeros((16, HD), F32)
            for j in range(GROUP):
                row = joined[base + g * GROUP + j : base + g * GROUP + j + 1]
                logical = jnp.where(logical_row == order_ref[j], row, logical)
            logical = logical * factor
            rotated = logical * cosines[b] + pltpu.roll(logical, HD // 2, 1) * sines[b]
            rotated = rotated.astype(BF16)
            queries = rotated[0:PER_GROUP]
            new_key = rotated.astype(F32)[PER_GROUP : PER_GROUP + 1]
            new_value = logical[PER_GROUP + 1 : PER_GROUP + 2].astype(BF16).astype(F32)
            own = jnp.sum(queries.astype(F32) * new_key, axis=1, keepdims=True)
            scores = lax.dot_general(
                queries, keys[b, g], (((1,), (1,)), ((), ())), preferred_element_type=F32
            )
            masked = jnp.where(position < len_ref[b], scores, -jnp.inf)
            peak = jnp.maximum(jnp.max(masked, axis=1, keepdims=True), own)
            weights = jnp.exp((masked - peak) * inv_scale)
            own_weight = jnp.exp((own - peak) * inv_scale)
            denom = jnp.sum(weights, axis=1, keepdims=True) + own_weight
            mixed = jnp.dot(weights.astype(BF16), values[b, g], preferred_element_type=F32)
            mixed = mixed + own_weight.astype(BF16).astype(F32) * new_value
            att_out[pl.ds((b * LOCAL_GROUPS + g) * PER_GROUP, PER_GROUP)] = mixed / denom

    att_in[rank] = att_out[...].astype(BF16)

    def send_attended(k, carry):
        other, device = peer(k)
        remote(att_in.at[rank], att_in.at[rank], 1, device).start()
        return carry

    lax.fori_loop(1, RANKS, send_attended, 0)
    wait_all(att_in.at[rest], att_in.at[rest], 1)

    def widen(i, carry):
        att32[pl.ds(i * SEQS, SEQS)] = att_in[i].astype(F32).reshape(SEQS, LOCAL_HEADS, HD)
        return carry

    lax.fori_loop(0, RANKS, widen, 0)
    loads[6].wait()
    attended = jnp.concatenate([att32[:, h, :].astype(BF16) for h in range(LOCAL_HEADS)], axis=1)
    partial = jnp.dot(attended, outw[...], preferred_element_type=F32)

    def sum_over_tensor(value, buffer, i):
        buffer[tensor] = value.astype(BF16)
        for k in range(1, TENSOR):
            remote(buffer.at[tensor], buffer.at[tensor], i, tensor_peer(k)).start()
        others = pl.ds(0, TENSOR - 1)
        whole = remote(buffer.at[others], buffer.at[others], i, tensor_peer(1))
        whole.wait_send()
        whole.wait_recv()
        total = buffer[0].astype(F32)
        for k in range(1, TENSOR):
            total = total + buffer[k].astype(F32)
        return total

    projected = sum_over_tensor(partial, proj1, 2)
    hidden = (tokens[...].astype(F32) + projected).astype(BF16).astype(F32)

    squares = jnp.sum(hidden * hidden, axis=1, keepdims=True)
    row_of = lax.broadcasted_iota(jnp.int32, (B, HD), 0)
    lane_of = lax.broadcasted_iota(jnp.int32, (B, HD), 1)
    sq_out[...] = jnp.sum(jnp.where(row_of == lane_of, squares, 0.0), axis=0, keepdims=True)
    sq_in[rank] = sq_out[...]

    def send_squares(k, carry):
        other, device = peer(k)
        remote(sq_out, sq_in.at[rank], 3, device).start()
        return carry

    lax.fori_loop(1, RANKS, send_squares, 0)
    scaled = (hidden * gains[1]).astype(BF16)
    loads[7].wait()

    def at(dx, dy, dz):
        x2, y2, z2 = lax.rem(x + dx, NX), lax.rem(dp + dy, NY), lax.rem(z + dz, NZ)
        return x2, y2, z2, {"section": x2 * NZ + z2, "dp": y2}

    def rows_of(y2):
        return pl.ds(pl.multiple_of(y2 * ROWS_EACH, ROWS_EACH), ROWS_EACH)

    own_rows = rows_of(dp)
    first_peers = {
        "x": [(2, 0, 0), (1, 0, 0), (3, 0, 0)],
        "y": [(0, 2, 0), (0, 1, 0), (0, 3, 0)],
        "z": [(0, 0, 1)],
    }
    second_peers = {
        "x": [(0, dy, dz) for dy in (2, 1, 3, 0) for dz in (1, 0) if dy or dz],
        "y": [(dx, 0, dz) for dx in (2, 1, 3, 0) for dz in (1, 0) if dx or dz],
        "z": [(dx, dy, 0) for dx in (2, 1, 3, 0) for dy in (2, 1, 3, 0) if dx or dy],
    }

    def send(i, src, dst, device):
        remote(src, dst, i, device).start()

    def wait_recv(i, like):
        remote(like, like, i, peer(1)[1]).wait_recv()

    def wait_send(i, like):
        remote(like, like, i, peer(1)[1]).wait_send()

    base = 7
    for p, (kind, first, count) in enumerate(CHUNKS):
        out, arrived = gu_out[p], gu_in1[p]
        width = count * 128
        for c in range(SECTIONS):
            for half in range(2):
                start = c * UNITS_EACH + first * 128
                product = jnp.dot(
                    scaled, gate_up[half, :, start : start + width], preferred_element_type=F32
                ).astype(BF16)
                if kind == "x":
                    out[c // NZ, c % NZ, half] = product
                elif kind == "y":
                    for y2 in range(NY):
                        out[y2, c, half] = product[y2 * ROWS_EACH : (y2 + 1) * ROWS_EACH]
                else:
                    out[c % NZ, c // NZ, half] = product
        for k, offset in enumerate(first_peers[kind]):
            x2, y2, z2, device = at(*offset)
            to = {"x": x2, "y": y2, "z": z2}[kind]
            send(base + p, out.at[to], arrived.at[k], device)
    for p, (kind, first, count) in enumerate(CHUNKS):
        out, arrived, total, arrived2 = gu_out[p], gu_in1[p], gu_sum[p], gu_in2[p]
        wait_recv(base + p, arrived)
        mine = {"x": x, "y": dp, "z": z}[kind]

        def add(i, carry):
            for half in range(2):
                value = out[mine, i, half].astype(F32)
                for k in range(len(first_peers[kind])):
                    value = value + arrived[k, i, half].astype(F32)
                total[i, half] = value.astype(BF16)
            return carry

        lax.fori_loop(0, total.shape[0], add, 0)
        for k, offset in enumerate(second_peers[kind]):
            x2, y2, z2, device = at(*offset)
            if kind == "x":
                src = total.at[z2, :, rows_of(y2)]
            elif kind == "y":
                src = total.at[x2 * NZ + z2]
            else:
                src = total.at[x2, :, rows_of(y2)]
            send(base + 5 + p, src, arrived2.at[k], device)

    wait_all(sq_in.at[rest], sq_in.at[rest], 3)
    total = jnp.sum(sq_in[...], axis=0)
    row_of = lax.broadcasted_iota(jnp.int32, (ROWS_EACH, HD), 0) + dp * ROWS_EACH
    lane_of = lax.broadcasted_iota(jnp.int32, (ROWS_EACH, HD), 1)
    total = jnp.sum(jnp.where(row_of == lane_of, total, 0.0), axis=1, keepdims=True)
    factor = lax.rsqrt(total / D + 1e-05)

    for p, (kind, first, count) in enumerate(CHUNKS):
        total, arrived2, part = gu_sum[p], gu_in2[p], act[p]
        wait_recv(base + 5 + p, arrived2)
        halves = []
        for half in range(2):
            if kind == "x":
                value = total[z, half, own_rows]
            elif kind == "y":
                value = total[section, half]
            else:
                value = total[x, half, own_rows]
            value = value.astype(F32)
            for k in range(len(second_peers[kind])):
                value = value + arrived2[k, half].astype(F32)
            halves.append(value * factor)
        gate, up = halves
        part[x, z, own_rows] = (gate / (1.0 + jnp.exp(-gate)) * up).astype(BF16)
        block = part.at[x, z, own_rows]
        for offset in second_peers[kind]:
            send(base + 10 + p, block, block, at(*offset)[3])
    for p, (kind, first, count) in enumerate(CHUNKS):
        part = act[p]
        wait_recv(base + 10 + p, gu_in2[p].at[:, 0])
        if kind == "x":
            block = part.at[x]
        elif kind == "y":
            block = part.at[:, :, own_rows]
        else:
            block = part.at[:, z]
        for offset in first_peers[kind]:
            send(base + 15 + p, block, block, at(*offset)[3])
    loads[8].wait()
    partial = jnp.zeros((B, COLS), F32)
    for p, (kind, first, count) in enumerate(CHUNKS):
        wait_recv(base + 15 + p, gu_in1[p].at[:, :, 0])
        width = count * 128
        for c in range(SECTIONS):
            start = c * UNITS_EACH + first * 128
            partial = partial + jnp.dot(
                act[p][c // NZ, c % NZ], down[start : start + width], preferred_element_type=F32
            )
    lowered = sum_over_tensor(partial, proj2, 6)
    for p in range(5):
        wait_send(base + p, gu_in1[p])
        wait_send(base + 5 + p, gu_in2[p])
        wait_send(base + 10 + p, gu_in2[p].at[:, 0])
        wait_send(base + 15 + p, gu_in1[p].at[:, :, 0])
    out_ref[...] = hidden + lowered


def chunk_buffers():
    out, in1, total, in2, act = [], [], [], [], []
    for kind, first, count in CHUNKS:
        w = count * 128
        ways, block, peers = {
            "x": (NX, (NZ, 2, B, w), 7),
            "y": (NY, (SECTIONS, 2, ROWS_EACH, w), 7),
            "z": (NZ, (NX, 2, B, w), 15),
        }[kind]
        out.append(pltpu.VMEM((ways, *block), BF16))
        in1.append(pltpu.VMEM((ways - 1, *block), BF16))
        total.append(pltpu.VMEM(block, BF16))
        in2.append(pltpu.VMEM((peers, 2, ROWS_EACH, w), BF16))
        act.append(pltpu.VMEM((NX, NZ, B, w), BF16))
    return [*out, *in1, *total, *in2, *act]


def body(
    tokens,
    attn_gain,
    qkv_weight,
    qkv_order,
    cache_keys,
    cache_values,
    cache_len,
    out_weight,
    ffn_gain,
    gate_up,
    down_weight,
):
    half_dim = HD // 2
    inv_freq = 500000.0 ** (-(2.0 * np.arange(half_dim)) / HD)
    inv_freq = np.concatenate([inv_freq, inv_freq])[None, :].astype(np.float32)
    hbm = pl.BlockSpec(memory_space=pl.ANY)
    out = pl.pallas_call(
        layer_kernel,
        out_shape=jax.ShapeDtypeStruct((B, COLS), F32),
        in_specs=[hbm] * 12,
        out_specs=pl.BlockSpec(memory_space=pltpu.VMEM),
        scratch_shapes=[
            pltpu.SMEM((GROUP,), jnp.int32),
            pltpu.SMEM((SEQS,), jnp.int32),
            pltpu.VMEM((1, HD), F32),
            pltpu.VMEM((B, COLS), BF16),
            pltpu.VMEM((2, 1, COLS), F32),
            pltpu.VMEM(qkv_weight.shape, BF16),
            pltpu.VMEM(cache_keys.shape, BF16),
            pltpu.VMEM(cache_values.shape, BF16),
            pltpu.VMEM(out_weight.shape, BF16),
            pltpu.VMEM(gate_up.shape, BF16),
            pltpu.VMEM(down_weight.shape, BF16),
            pltpu.VMEM((B, SLOT_ROWS, HD), F32),
            pltpu.VMEM((RANKS, SEQS * SLOT_ROWS, HD), BF16),
            pltpu.VMEM((RANKS, SEQS * SLOT_ROWS, HD), BF16),
            pltpu.VMEM((SEQS * LOCAL_HEADS, HD), F32),
            pltpu.VMEM((RANKS, SEQS * LOCAL_HEADS, HD), BF16),
            pltpu.VMEM((B, LOCAL_HEADS, HD), F32),
            pltpu.VMEM((TENSOR, B, COLS), BF16),
            pltpu.VMEM((TENSOR, B, COLS), BF16),
            pltpu.VMEM((1, 128), F32),
            pltpu.VMEM((RANKS, 1, 128), F32),
            *chunk_buffers(),
            pltpu.SemaphoreType.DMA((12,)),
            pltpu.SemaphoreType.DMA((27,)),
            pltpu.SemaphoreType.DMA((27,)),
        ],
        compiler_params=pltpu.CompilerParams(
            collective_id=0, has_side_effects=True, vmem_limit_bytes=60 * 2**20
        ),
        name="decoder_layer",
    )(
        qkv_order,
        cache_len,
        inv_freq,
        tokens,
        attn_gain.reshape(1, COLS),
        ffn_gain.reshape(1, COLS),
        qkv_weight,
        cache_keys,
        cache_values,
        out_weight,
        gate_up,
        down_weight,
    )
    return out.astype(BF16)


def solution(mesh):
    rows = P(None, ("section", "dp"))
    return jax.shard_map(
        body,
        mesh=mesh,
        in_specs=(
            rows,
            P(("section", "dp")),
            P(("section", "dp"), "tensor"),
            P(),
            P(("section", "dp"), "tensor", None, None),
            P(("section", "dp"), "tensor", None, None),
            P(("section", "dp")),
            P("tensor", ("section", "dp")),
            P(("section", "dp")),
            P(None, ("section", "dp"), "tensor"),
            P("tensor", ("section", "dp")),
        ),
        out_specs=rows,
        check_vma=False,
    )
```

```python
import jax
import jax.numpy as jnp
import numpy as np
from jax import lax
from jax.experimental import pallas as pl
from jax.experimental.pallas import tpu as pltpu
from jax.sharding import PartitionSpec as P

D = 4096
HEADS = 64
KV_HEADS = 8
HD = 128
FF = 28672
LEN = 4096
GROUP = 10
B = 64
RANKS = 32
TENSOR = 4
DP = 4
SEQS = B // RANKS
LOCAL_GROUPS = KV_HEADS // TENSOR
PER_GROUP = HEADS // KV_HEADS
COLS = D // RANKS
SLOT_ROWS = 24
LOCAL_HEADS = HEADS // TENSOR
UNITS = FF // TENSOR
SECTIONS = 8
NX, NY, NZ = 4, 4, 2
ROWS_EACH = B // NY
UNITS_EACH = UNITS // SECTIONS
FAR_FIRST = sorted(
    [(dx, dy, dz) for dx in range(NX) for dy in range(NY) for dz in range(NZ) if dx or dy or dz],
    key=lambda o: -(min(o[0], NX - o[0]) + min(o[1], NY - o[1]) + 2 * o[2]),
)
CHUNKS = (("x", 0, 2), ("y", 2, 2), ("z", 4, 1), ("x", 5, 1), ("y", 6, 1))
MESH = pl.DeviceIdType.MESH
F32 = jnp.float32
BF16 = jnp.bfloat16


def layer_kernel(
    order_hbm,
    len_hbm,
    freq_hbm,
    tokens_hbm,
    gain1_hbm,
    gain2_hbm,
    qkv_hbm,
    keys_hbm,
    values_hbm,
    outw_hbm,
    gate_up_hbm,
    down_hbm,
    out_ref,
    order_ref,
    len_ref,
    freq,
    tokens,
    gains,
    qkvw,
    keys,
    values,
    outw,
    gate_up,
    down,
    joined32,
    joined_out,
    joined_in,
    att_out,
    att_in,
    att32,
    proj1,
    proj2,
    sq_out,
    sq_in,
    *rest_refs,
):
    gu_out, gu_in1, gu_passed, gu_sum, gu_in2, act = (rest_refs[5 * i : 5 * i + 5] for i in range(6))
    lowered_sum, load_sem, send_sem, recv_sem = rest_refs[30:]
    section = lax.axis_index("section")
    x = section // NZ
    z = lax.rem(section, NZ)
    dp = lax.axis_index("dp")
    tensor = lax.axis_index("tensor")
    rank = section * DP + dp

    def load(i, src, dst):
        return pltpu.make_async_copy(src, dst, load_sem.at[i])

    loads = [
        load(0, tokens_hbm, tokens),
        load(1, gain1_hbm, gains.at[0]),
        load(2, qkv_hbm, qkvw),
        load(3, freq_hbm, freq),
        load(4, keys_hbm, keys),
        load(5, values_hbm, values),
        load(6, outw_hbm, outw),
        load(7, gate_up_hbm, gate_up),
        load(8, down_hbm, down),
        load(9, gain2_hbm, gains.at[1]),
        load(10, order_hbm, order_ref),
        load(11, len_hbm, len_ref),
    ]
    def at(dx, dy, dz):
        x2, y2, z2 = lax.rem(x + dx, NX), lax.rem(dp + dy, NY), lax.rem(z + dz, NZ)
        return x2, y2, z2, {"section": x2 * NZ + z2, "dp": y2}

    def peer(offset):
        x2, y2, z2, device = at(*offset)
        return (x2 * NZ + z2) * DP + y2, device

    def tensor_peer(k):
        return {"tensor": lax.rem(tensor + k, TENSOR)}

    barrier = pltpu.get_barrier_semaphore()

    for offset in FAR_FIRST:
        pl.semaphore_signal(barrier, inc=1, device_id=peer(offset)[1], device_id_type=MESH)
    for k in range(1, TENSOR):
        pl.semaphore_signal(barrier, inc=1, device_id=tensor_peer(k), device_id_type=MESH)

    for copy in loads:
        copy.start()

    loads[0].wait()
    loads[1].wait()
    wide = tokens[...].astype(F32)
    squares = jnp.sum(wide * wide, axis=1, keepdims=True)
    left = jnp.broadcast_to(squares, (B, HD))
    for i in range(3):
        part = left.astype(BF16).astype(F32)
        joined32[pl.Slice(20 + i, B, SLOT_ROWS)] = part
        left = left - part
    joined32[pl.Slice(23, B, SLOT_ROWS)] = jnp.zeros((B, HD), F32)
    scaled = (wide * gains[0]).astype(BF16)
    loads[2].wait()
    for j in range(LOCAL_GROUPS * GROUP // 2):
        product = jnp.dot(scaled, qkvw[:, j * 256 : j * 256 + 256], preferred_element_type=F32)
        joined32[pl.Slice(2 * j, B, SLOT_ROWS)] = product[:, :HD]
        joined32[pl.Slice(2 * j + 1, B, SLOT_ROWS)] = product[:, HD:]

    def pack(i, carry):
        joined_out[i] = joined32[pl.ds(i * SEQS * SLOT_ROWS, SEQS * SLOT_ROWS)].astype(BF16)
        return carry

    lax.fori_loop(0, RANKS, pack, 0)
    for i in (3, 9, 10, 11):
        loads[i].wait()
    low = lax.broadcasted_iota(jnp.int32, (1, HD), 1) < HD // 2
    cosines, sines = [], []
    for b in range(SEQS):
        angle = freq[...] * len_ref[b].astype(F32)
        cosines.append(jnp.cos(angle))
        sine = jnp.sin(angle)
        sines.append(jnp.where(low, -sine, sine))
    joined_in[rank] = joined_out[rank]

    pl.semaphore_wait(barrier, RANKS - 1 + TENSOR - 1)

    def remote(src, dst, i, device):
        return pltpu.make_async_remote_copy(
            src_ref=src,
            dst_ref=dst,
            send_sem=send_sem.at[i],
            recv_sem=recv_sem.at[i],
            device_id=device,
            device_id_type=MESH,
        )

    for offset in FAR_FIRST:
        other, device = peer(offset)
        remote(joined_out.at[other], joined_in.at[rank], 0, device).start()

    def wait_all(src, dst, i):
        whole = remote(src, dst, i, peer(FAR_FIRST[-1])[1])
        whole.wait_send()
        whole.wait_recv()

    rest = pl.ds(0, RANKS - 1)
    wait_all(joined_out.at[rest], joined_in.at[rest], 0)

    joined = joined_in[0].astype(F32)
    for i in range(1, RANKS):
        joined = joined + joined_in[i].astype(F32)

    loads[4].wait()
    loads[5].wait()
    inv_scale = HD**-0.5
    position = lax.broadcasted_iota(jnp.int32, (PER_GROUP, LEN), 1)
    logical_row = lax.broadcasted_iota(jnp.int32, (16, HD), 0)
    for b in range(SEQS):
        base = b * SLOT_ROWS
        total = joined[base + 20 : base + 21] + joined[base + 21 : base + 22] + joined[base + 22 : base + 23]
        factor = lax.rsqrt(total / D + 1e-05)
        for g in range(LOCAL_GROUPS):
            logical = jnp.zeros((16, HD), F32)
            for j in range(GROUP):
                row = joined[base + g * GROUP + j : base + g * GROUP + j + 1]
                logical = jnp.where(logical_row == order_ref[j], row, logical)
            logical = logical * factor
            rotated = logical * cosines[b] + pltpu.roll(logical, HD // 2, 1) * sines[b]
            rotated = rotated.astype(BF16)
            queries = rotated[0:PER_GROUP]
            new_key = rotated.astype(F32)[PER_GROUP : PER_GROUP + 1]
            new_value = logical[PER_GROUP + 1 : PER_GROUP + 2].astype(BF16).astype(F32)
            own = jnp.sum(queries.astype(F32) * new_key, axis=1, keepdims=True)
            scores = lax.dot_general(
                queries, keys[b, g], (((1,), (1,)), ((), ())), preferred_element_type=F32
            )
            masked = jnp.where(position < len_ref[b], scores, -jnp.inf)
            peak = jnp.maximum(jnp.max(masked, axis=1, keepdims=True), own)
            weights = jnp.exp((masked - peak) * inv_scale)
            own_weight = jnp.exp((own - peak) * inv_scale)
            denom = jnp.sum(weights, axis=1, keepdims=True) + own_weight
            mixed = jnp.dot(weights.astype(BF16), values[b, g], preferred_element_type=F32)
            mixed = mixed + own_weight.astype(BF16).astype(F32) * new_value
            att_out[pl.ds((b * LOCAL_GROUPS + g) * PER_GROUP, PER_GROUP)] = mixed / denom

    att_in[rank] = att_out[...].astype(BF16)

    for offset in FAR_FIRST:
        remote(att_in.at[rank], att_in.at[rank], 1, peer(offset)[1]).start()
    wait_all(att_in.at[rest], att_in.at[rest], 1)

    def widen(i, carry):
        att32[pl.ds(i * SEQS * LOCAL_HEADS, SEQS * LOCAL_HEADS)] = att_in[i].astype(F32)
        return carry

    lax.fori_loop(0, RANKS, widen, 0)
    loads[6].wait()
    attended = jnp.concatenate([att32[pl.Slice(h, B, LOCAL_HEADS)].astype(BF16) for h in range(LOCAL_HEADS)], axis=1)
    partial = jnp.dot(attended, outw[...], preferred_element_type=F32)

    def sum_over_tensor(value, buffer, i):
        buffer[tensor] = value.astype(BF16)
        for k in range(1, TENSOR):
            remote(buffer.at[tensor], buffer.at[tensor], i, tensor_peer(k)).start()
        others = pl.ds(0, TENSOR - 1)
        whole = remote(buffer.at[others], buffer.at[others], i, tensor_peer(1))
        whole.wait_send()
        whole.wait_recv()
        total = buffer[0].astype(F32)
        for k in range(1, TENSOR):
            total = total + buffer[k].astype(F32)
        return total

    projected = sum_over_tensor(partial, proj1, 2)
    hidden = (tokens[...].astype(F32) + projected).astype(BF16).astype(F32)

    squares = jnp.sum(hidden * hidden, axis=1, keepdims=True)
    row_of = lax.broadcasted_iota(jnp.int32, (B, HD), 0)
    lane_of = lax.broadcasted_iota(jnp.int32, (B, HD), 1)
    sq_out[...] = jnp.sum(jnp.where(row_of == lane_of, squares, 0.0), axis=0, keepdims=True)
    sq_in[rank] = sq_out[...]

    for offset in FAR_FIRST:
        remote(sq_out, sq_in.at[rank], 3, peer(offset)[1]).start()
    scaled = (hidden * gains[1]).astype(BF16)
    loads[7].wait()

    def rows_of(y2):
        return pl.ds(pl.multiple_of(y2 * ROWS_EACH, ROWS_EACH), ROWS_EACH)

    own_rows = rows_of(dp)
    ring = {"x": [(1, 0, 0), (3, 0, 0), (2, 0, 0)], "y": [(0, 1, 0), (0, 3, 0), (0, 2, 0)]}
    first_peers = {
        "x": [(2, 0, 0), (1, 0, 0), (3, 0, 0)],
        "y": [(0, 2, 0), (0, 1, 0), (0, 3, 0)],
        "z": [(0, 0, 1)],
    }
    second_peers = {
        "x": [(0, dy, dz) for dy in (2, 1, 3, 0) for dz in (1, 0) if dy or dz],
        "y": [(dx, 0, dz) for dx in (2, 1, 3, 0) for dz in (1, 0) if dx or dz],
        "z": [(dx, dy, 0) for dx in (2, 1, 3, 0) for dy in (2, 1, 3, 0) if dx or dy],
    }

    def send(i, src, dst, device):
        remote(src, dst, i, device).start()

    def wait_recv(i, like):
        remote(like, like, i, peer(FAR_FIRST[-1])[1]).wait_recv()

    def wait_send(i, like):
        remote(like, like, i, peer(FAR_FIRST[-1])[1]).wait_send()

    base = 7
    step_a, step_b, step_c, step_2, step_3, step_4 = (base + 5 * i for i in range(6))
    for p, (kind, first, count) in enumerate(CHUNKS):
        out, arrived = gu_out[p], gu_in1[p]
        width = count * 128
        for c in range(SECTIONS):
            for half in range(2):
                start = c * UNITS_EACH + first * 128
                product = jnp.dot(
                    scaled, gate_up[half, :, start : start + width], preferred_element_type=F32
                ).astype(BF16)
                if kind == "x":
                    out[c // NZ, c % NZ, half] = product
                elif kind == "y":
                    for y2 in range(NY):
                        out[y2, c // 4, c % 4, half] = product[y2 * ROWS_EACH : (y2 + 1) * ROWS_EACH]
                else:
                    out[c % NZ, c // NZ, half] = product
        if kind == "z":
            _, _, z2, device = at(0, 0, 1)
            send(step_a + p, out.at[z2], arrived.at[0], device)
            continue
        along = 0 if kind == "x" else 1
        after, before, across = ring[kind]
        far, right, left = at(*across)[along], at(*after), at(*before)
        send(step_a + p, out.at[far, 0], arrived.at[0, 0], right[3])
        send(step_a + p, out.at[far, 1], arrived.at[0, 1], left[3])
        send(step_b + p, out.at[right[along], 1], arrived.at[1, 1], right[3])
        send(step_b + p, out.at[left[along], 0], arrived.at[1, 0], left[3])
    for p, (kind, first, count) in enumerate(CHUNKS):
        if kind == "z":
            continue
        out, arrived = gu_out[p], gu_in1[p]
        along = 0 if kind == "x" else 1
        after, before, _ = ring[kind]
        right, left = at(*after), at(*before)
        wait_recv(step_a + p, arrived.at[0])
        passed = gu_passed[p]
        for i, (to, device) in enumerate(((right[along], right[3]), (left[along], left[3]))):

            def merge(j, carry):
                passed[i, j] = (out[to, i, j].astype(F32) + arrived[0, i, j].astype(F32)).astype(BF16)
                return carry

            lax.fori_loop(0, passed.shape[1], merge, 0, unroll=True)
            send(step_c + p, passed.at[i], arrived.at[2, i], device)
    for p, (kind, first, count) in enumerate(CHUNKS):
        out, arrived, total, arrived2 = gu_out[p], gu_in1[p], gu_sum[p], gu_in2[p]
        if kind == "z":
            wait_recv(step_a + p, arrived)

            def add(i, carry):
                total[i] = (out[z, i].astype(F32) + arrived[0, i].astype(F32)).astype(BF16)
                return carry

            lax.fori_loop(0, total.shape[0], add, 0)
        else:
            wait_recv(step_b + p, arrived.at[1])
            wait_recv(step_c + p, arrived.at[2])
            mine = x if kind == "x" else dp
            for i in range(2):

                def add(j, carry):
                    value = out[mine, i, j].astype(F32) + arrived[1, i, j].astype(F32)
                    total[i, j] = (value + arrived[2, i, j].astype(F32)).astype(BF16)
                    return carry

                lax.fori_loop(0, total.shape[1], add, 0, unroll=True)
        for k, offset in enumerate(second_peers[kind]):
            x2, y2, z2, device = at(*offset)
            if kind == "x":
                src = total.at[z2, :, rows_of(y2)]
            elif kind == "y":
                src = total.at[x2 // 2, lax.rem(x2, 2) * NZ + z2]
            else:
                src = total.at[x2, :, rows_of(y2)]
            send(step_2 + p, src, arrived2.at[k], device)

    wait_all(sq_in.at[rest], sq_in.at[rest], 3)
    total = jnp.sum(sq_in[...], axis=0)
    row_of = lax.broadcasted_iota(jnp.int32, (ROWS_EACH, HD), 0) + dp * ROWS_EACH
    lane_of = lax.broadcasted_iota(jnp.int32, (ROWS_EACH, HD), 1)
    total = jnp.sum(jnp.where(row_of == lane_of, total, 0.0), axis=1, keepdims=True)
    factor = lax.rsqrt(total / D + 1e-05)

    def like_3(p):
        return gu_in2[p].at[:, 0]

    def like_4(p):
        return gu_in1[p].at[0, :, 0] if CHUNKS[p][0] == "z" else gu_in1[p].at[:, 0]

    def activate(p):
        kind = CHUNKS[p][0]
        total, arrived2, part = gu_sum[p], gu_in2[p], act[p]
        wait_recv(step_2 + p, arrived2)
        halves = []
        for half in range(2):
            if kind == "x":
                value = total[z, half, own_rows]
            elif kind == "y":
                value = total[x // 2, lax.rem(x, 2) * NZ + z, half]
            else:
                value = total[x, half, own_rows]
            value = value.astype(F32)
            for k in range(len(second_peers[kind])):
                value = value + arrived2[k, half].astype(F32)
            halves.append(value * factor)
        gate, up = halves
        part[x, z, own_rows] = (gate / (1.0 + jnp.exp(-gate)) * up).astype(BF16)
        block = part.at[x, z, own_rows]
        for offset in second_peers[kind]:
            send(step_3 + p, block, block, at(*offset)[3])

    def pass_on(p):
        kind = CHUNKS[p][0]
        part = act[p]
        wait_recv(step_3 + p, like_3(p))
        if kind == "x":
            block = part.at[x]
        elif kind == "y":
            block = part.at[:, :, own_rows]
        else:
            block = part.at[:, z]
        for offset in first_peers[kind]:
            send(step_4 + p, block, block, at(*offset)[3])

    def lower(p):
        kind, first, count = CHUNKS[p]
        wait_recv(step_4 + p, like_4(p))
        width = count * 128
        partial = None
        for c in range(SECTIONS):
            start = c * UNITS_EACH + first * 128
            product = jnp.dot(
                act[p][c // NZ, c % NZ], down[start : start + width], preferred_element_type=F32
            )
            partial = product if partial is None else partial + product
        lowered_sum[...] = partial if p == 0 else lowered_sum[...] + partial

    for p in range(5):
        activate(p)
    for p in range(5):
        pass_on(p)
    loads[8].wait()
    for p in range(5):
        lower(p)
    partial = lowered_sum[...]
    lowered = sum_over_tensor(partial, proj2, 6)
    for p in range(5):
        if CHUNKS[p][0] == "z":
            wait_send(step_a + p, gu_in1[p])
        else:
            for i, step in enumerate((step_a, step_b, step_c)):
                wait_send(step + p, gu_in1[p].at[i])
        wait_send(step_2 + p, gu_in2[p])
        wait_send(step_3 + p, like_3(p))
        wait_send(step_4 + p, like_4(p))
    out_ref[...] = hidden + lowered


def chunk_buffers():
    out, in1, passed, total, in2, act = [], [], [], [], [], []
    for kind, first, count in CHUNKS:
        w = count * 128
        if kind == "z":
            shape, arrived, peers = (NX, 2, B, w), (1, NX, 2, B, w), NX * NY - 1
            kept = (8, w)
        else:
            shape = {"x": (2, 2, B, w), "y": (2, 4, 2, ROWS_EACH, w)}[kind]
            arrived, kept, peers = (3, *shape), shape, 7
        out.append(pltpu.VMEM(({"x": NX, "y": NY, "z": NZ}[kind], *shape), BF16))
        in1.append(pltpu.VMEM(arrived, BF16))
        passed.append(pltpu.VMEM(kept, BF16))
        total.append(pltpu.VMEM(shape, BF16))
        in2.append(pltpu.VMEM((peers, 2, ROWS_EACH, w), BF16))
        act.append(pltpu.VMEM((NX, NZ, B, w), BF16))
    return [*out, *in1, *passed, *total, *in2, *act, pltpu.VMEM((B, COLS), F32)]


def body(
    tokens,
    attn_gain,
    qkv_weight,
    qkv_order,
    cache_keys,
    cache_values,
    cache_len,
    out_weight,
    ffn_gain,
    gate_up,
    down_weight,
):
    half_dim = HD // 2
    inv_freq = 500000.0 ** (-(2.0 * np.arange(half_dim)) / HD)
    inv_freq = np.concatenate([inv_freq, inv_freq])[None, :].astype(np.float32)
    hbm = pl.BlockSpec(memory_space=pl.ANY)
    out = pl.pallas_call(
        layer_kernel,
        out_shape=jax.ShapeDtypeStruct((B, COLS), F32),
        in_specs=[hbm] * 12,
        out_specs=pl.BlockSpec(memory_space=pltpu.VMEM),
        scratch_shapes=[
            pltpu.SMEM((GROUP,), jnp.int32),
            pltpu.SMEM((SEQS,), jnp.int32),
            pltpu.VMEM((1, HD), F32),
            pltpu.VMEM((B, COLS), BF16),
            pltpu.VMEM((2, 1, COLS), F32),
            pltpu.VMEM(qkv_weight.shape, BF16),
            pltpu.VMEM(cache_keys.shape, BF16),
            pltpu.VMEM(cache_values.shape, BF16),
            pltpu.VMEM(out_weight.shape, BF16),
            pltpu.VMEM(gate_up.shape, BF16),
            pltpu.VMEM(down_weight.shape, BF16),
            pltpu.VMEM((B * SLOT_ROWS, HD), F32),
            pltpu.VMEM((RANKS, SEQS * SLOT_ROWS, HD), BF16),
            pltpu.VMEM((RANKS, SEQS * SLOT_ROWS, HD), BF16),
            pltpu.VMEM((SEQS * LOCAL_HEADS, HD), F32),
            pltpu.VMEM((RANKS, SEQS * LOCAL_HEADS, HD), BF16),
            pltpu.VMEM((B * LOCAL_HEADS, HD), F32),
            pltpu.VMEM((TENSOR, B, COLS), BF16),
            pltpu.VMEM((TENSOR, B, COLS), BF16),
            pltpu.VMEM((1, 128), F32),
            pltpu.VMEM((RANKS, 1, 128), F32),
            *chunk_buffers(),
            pltpu.SemaphoreType.DMA((12,)),
            pltpu.SemaphoreType.DMA((37,)),
            pltpu.SemaphoreType.DMA((37,)),
        ],
        compiler_params=pltpu.CompilerParams(
            collective_id=0, has_side_effects=True, vmem_limit_bytes=32 * 2**20
        ),
        name="decoder_layer",
    )(
        *(
            pltpu.with_memory_space_constraint(operand, pltpu.HBM)
            for operand in (
                qkv_order,
                cache_len,
                jnp.asarray(inv_freq),
                tokens,
                attn_gain.reshape(1, COLS),
                ffn_gain.reshape(1, COLS),
                qkv_weight,
                cache_keys,
                cache_values,
                out_weight,
                gate_up,
                down_weight,
            )
        )
    )
    return out.astype(BF16)


def solution(mesh):
    rows = P(None, ("section", "dp"))
    return jax.shard_map(
        body,
        mesh=mesh,
        in_specs=(
            rows,
            P(("section", "dp")),
            P(("section", "dp"), "tensor"),
            P(),
            P(("section", "dp"), "tensor", None, None),
            P(("section", "dp"), "tensor", None, None),
            P(("section", "dp")),
            P("tensor", ("section", "dp")),
            P(("section", "dp")),
            P(None, ("section", "dp"), "tensor"),
            P("tensor", ("section", "dp")),
        ),
        out_specs=rows,
        check_vma=False,
    )
```

```python
import jax
import jax.numpy as jnp
import numpy as np
from jax import lax
from jax.experimental import pallas as pl
from jax.experimental.pallas import tpu as pltpu
from jax.sharding import PartitionSpec as P

D = 4096
HEADS = 64
KV_HEADS = 8
HD = 128
FF = 28672
LEN = 4096
GROUP = 10
B = 64
RANKS = 32
TENSOR = 4
DP = 4
SEQS = B // RANKS
LOCAL_GROUPS = KV_HEADS // TENSOR
PER_GROUP = HEADS // KV_HEADS
COLS = D // RANKS
SLOT_ROWS = 24
LOCAL_HEADS = HEADS // TENSOR
UNITS = FF // TENSOR
SECTIONS = 8
NX, NY, NZ = 4, 4, 2
ROWS_EACH = B // NY
UNITS_EACH = UNITS // SECTIONS
FAR_FIRST = sorted(
    [(dx, dy, dz) for dx in range(NX) for dy in range(NY) for dz in range(NZ) if dx or dy or dz],
    key=lambda o: -(min(o[0], NX - o[0]) + min(o[1], NY - o[1]) + 2 * o[2]),
)
CHUNKS = (("x", 0, 3), ("y", 3, 2), ("z", 5, 2))
N_CHUNKS = len(CHUNKS)
WAYS = {"x": NX, "y": NY, "z": NZ}
BATCHES = {"x": (6, 4, 2), "y": (6, 4, 2), "z": (4, 2, 2)}
MESH = pl.DeviceIdType.MESH
F32 = jnp.float32
BF16 = jnp.bfloat16


def layer_kernel(
    order_hbm,
    len_hbm,
    freq_hbm,
    tokens_hbm,
    gain1_hbm,
    gain2_hbm,
    qkv_hbm,
    keys_hbm,
    values_hbm,
    outw_hbm,
    gate_up_hbm,
    down_hbm,
    out_ref,
    order_ref,
    len_ref,
    freq,
    tokens,
    gains,
    qkvw,
    keys,
    values,
    outw,
    down,
    joined32,
    joined_out,
    joined_in,
    att_out,
    att_in,
    att32,
    proj1,
    proj2,
    sq_out,
    sq_in,
    *rest_refs,
):
    wide_weights, wide_rows, gu_sum, gu_in2, act = (rest_refs[N_CHUNKS * i : N_CHUNKS * (i + 1)] for i in range(5))
    lowered_sum, own_rows_sem, load_sem, send_sem, recv_sem = rest_refs[5 * N_CHUNKS :]
    section = lax.axis_index("section")
    x = section // NZ
    z = lax.rem(section, NZ)
    dp = lax.axis_index("dp")
    tensor = lax.axis_index("tensor")
    rank = section * DP + dp

    def load(i, src, dst):
        return pltpu.make_async_copy(src, dst, load_sem.at[i])

    loads = {
        0: load(0, tokens_hbm, tokens),
        1: load(1, gain1_hbm, gains.at[0]),
        2: load(2, qkv_hbm, qkvw),
        3: load(3, freq_hbm, freq),
        9: load(9, gain2_hbm, gains.at[1]),
        10: load(10, order_hbm, order_ref),
        11: load(11, len_hbm, len_ref),
        4: load(4, keys_hbm, keys),
        5: load(5, values_hbm, values),
        6: load(6, outw_hbm, outw),
        8: load(8, down_hbm, down),
    }
    def at(dx, dy, dz):
        x2, y2, z2 = lax.rem(x + dx, NX), lax.rem(dp + dy, NY), lax.rem(z + dz, NZ)
        return x2, y2, z2, {"section": x2 * NZ + z2, "dp": y2}

    def peer(offset):
        x2, y2, z2, device = at(*offset)
        return (x2 * NZ + z2) * DP + y2, device

    def tensor_peer(k):
        return {"tensor": lax.rem(tensor + k, TENSOR)}

    barrier = pltpu.get_barrier_semaphore()

    for offset in FAR_FIRST:
        pl.semaphore_signal(barrier, inc=1, device_id=peer(offset)[1], device_id_type=MESH)
    for k in range(1, TENSOR):
        pl.semaphore_signal(barrier, inc=1, device_id=tensor_peer(k), device_id_type=MESH)

    for copy in loads.values():
        copy.start()

    loads[0].wait()
    loads[1].wait()
    wide = tokens[...].astype(F32)
    squares = jnp.sum(wide * wide, axis=1, keepdims=True)
    left = jnp.broadcast_to(squares, (B, HD))
    for i in range(3):
        part = left.astype(BF16).astype(F32)
        joined32[pl.Slice(20 + i, B, SLOT_ROWS)] = part
        left = left - part
    joined32[pl.Slice(23, B, SLOT_ROWS)] = jnp.zeros((B, HD), F32)
    scaled = (wide * gains[0]).astype(BF16)
    loads[2].wait()
    for j in range(LOCAL_GROUPS * GROUP // 2):
        product = jnp.dot(scaled, qkvw[:, j * 256 : j * 256 + 256], preferred_element_type=F32)
        joined32[pl.Slice(2 * j, B, SLOT_ROWS)] = product[:, :HD]
        joined32[pl.Slice(2 * j + 1, B, SLOT_ROWS)] = product[:, HD:]

    def pack(i, carry):
        joined_out[i] = joined32[pl.ds(i * SEQS * SLOT_ROWS, SEQS * SLOT_ROWS)].astype(BF16)
        return carry

    lax.fori_loop(0, RANKS, pack, 0)
    for i in (3, 9, 10, 11):
        loads[i].wait()
    low = lax.broadcasted_iota(jnp.int32, (1, HD), 1) < HD // 2
    cosines, sines = [], []
    for b in range(SEQS):
        angle = freq[...] * len_ref[b].astype(F32)
        cosines.append(jnp.cos(angle))
        sine = jnp.sin(angle)
        sines.append(jnp.where(low, -sine, sine))
    joined_in[rank] = joined_out[rank]

    pl.semaphore_wait(barrier, RANKS - 1 + TENSOR - 1)

    def remote(src, dst, i, device):
        return pltpu.make_async_remote_copy(
            src_ref=src,
            dst_ref=dst,
            send_sem=send_sem.at[i],
            recv_sem=recv_sem.at[i],
            device_id=device,
            device_id_type=MESH,
        )

    ring = {
        "x": [(2, 0, 0), (1, 0, 0), (3, 0, 0)],
        "y": [(0, 2, 0), (0, 1, 0), (0, 3, 0)],
        "z": [(0, 0, 1)],
    }

    def block_start(p, major, minor):
        return pl.multiple_of((major * NZ + minor) * UNITS_EACH + CHUNKS[p][1] * 128, 128)

    def weight_piece(p, to, i, half):
        kind, _, count = CHUNKS[p]
        start = block_start(p, i, to) if kind == "z" else block_start(p, to, i)
        return gate_up_hbm.at[half, :, pl.ds(start, count * 128)]

    def step_of(offset):
        return max(offset)

    place = {"x": x, "y": dp, "z": z}
    pieces = {}
    for p, (kind, _, _) in enumerate(CHUNKS):
        pieces[p] = [
            (offset, i, half) for i in range(NX if kind == "z" else NZ) for half in range(2) for offset in ring[kind]
        ]
        for i in range(NX if kind == "z" else NZ):
            for half in range(2):
                pltpu.make_async_copy(
                    weight_piece(p, place[kind], i, half), wide_weights[p].at[i, half, pl.ds(0, 128)], own_rows_sem.at[p]
                ).start()

    def send_weights(batch):
        for p, (kind, _, _) in enumerate(CHUNKS):
            first = sum(BATCHES[kind][:batch])
            for offset, i, half in pieces[p][first : first + BATCHES[kind][batch]]:
                to = at(*offset)
                dst = wide_weights[p].at[i, half, pl.ds(step_of(offset) * 128, 128)]
                remote(weight_piece(p, to["xyz".index(kind)], i, half), dst, 7 + p, to[3]).start()

    for offset in FAR_FIRST:
        other, device = peer(offset)
        remote(joined_out.at[other], joined_in.at[rank], 0, device).start()
    send_weights(0)

    def wait_all(src, dst, i):
        whole = remote(src, dst, i, peer(FAR_FIRST[-1])[1])
        whole.wait_send()
        whole.wait_recv()

    rest = pl.ds(0, RANKS - 1)
    wait_all(joined_out.at[rest], joined_in.at[rest], 0)

    joined = joined_in[0].astype(F32)
    for i in range(1, RANKS):
        joined = joined + joined_in[i].astype(F32)

    loads[4].wait()
    loads[5].wait()
    inv_scale = HD**-0.5
    position = lax.broadcasted_iota(jnp.int32, (PER_GROUP, LEN), 1)
    logical_row = lax.broadcasted_iota(jnp.int32, (16, HD), 0)
    for b in range(SEQS):
        base = b * SLOT_ROWS
        total = joined[base + 20 : base + 21] + joined[base + 21 : base + 22] + joined[base + 22 : base + 23]
        factor = lax.rsqrt(total / D + 1e-05)
        for g in range(LOCAL_GROUPS):
            logical = jnp.zeros((16, HD), F32)
            for j in range(GROUP):
                row = joined[base + g * GROUP + j : base + g * GROUP + j + 1]
                logical = jnp.where(logical_row == order_ref[j], row, logical)
            logical = logical * factor
            rotated = logical * cosines[b] + pltpu.roll(logical, HD // 2, 1) * sines[b]
            rotated = rotated.astype(BF16)
            queries = rotated[0:PER_GROUP]
            new_key = rotated.astype(F32)[PER_GROUP : PER_GROUP + 1]
            new_value = logical[PER_GROUP + 1 : PER_GROUP + 2].astype(BF16).astype(F32)
            own = jnp.sum(queries.astype(F32) * new_key, axis=1, keepdims=True)
            scores = lax.dot_general(
                queries, keys[b, g], (((1,), (1,)), ((), ())), preferred_element_type=F32
            )
            masked = jnp.where(position < len_ref[b], scores, -jnp.inf)
            peak = jnp.maximum(jnp.max(masked, axis=1, keepdims=True), own)
            weights = jnp.exp((masked - peak) * inv_scale)
            own_weight = jnp.exp((own - peak) * inv_scale)
            denom = jnp.sum(weights, axis=1, keepdims=True) + own_weight
            mixed = jnp.dot(weights.astype(BF16), values[b, g], preferred_element_type=F32)
            mixed = mixed + own_weight.astype(BF16).astype(F32) * new_value
            att_out[pl.ds((b * LOCAL_GROUPS + g) * PER_GROUP, PER_GROUP)] = mixed / denom

    att_in[rank] = att_out[...].astype(BF16)

    for offset in FAR_FIRST:
        remote(att_in.at[rank], att_in.at[rank], 1, peer(offset)[1]).start()
    send_weights(1)
    wait_all(att_in.at[rest], att_in.at[rest], 1)

    def widen(i, carry):
        att32[pl.ds(i * SEQS * LOCAL_HEADS, SEQS * LOCAL_HEADS)] = att_in[i].astype(F32)
        return carry

    lax.fori_loop(0, RANKS, widen, 0)
    loads[6].wait()
    attended = jnp.concatenate([att32[pl.Slice(h, B, LOCAL_HEADS)].astype(BF16) for h in range(LOCAL_HEADS)], axis=1)
    partial = jnp.dot(attended, outw[...], preferred_element_type=F32)

    def sum_over_tensor(value, buffer, i, then=lambda: None):
        buffer[tensor] = value.astype(BF16)
        for k in range(1, TENSOR):
            remote(buffer.at[tensor], buffer.at[tensor], i, tensor_peer(k)).start()
        then()
        others = pl.ds(0, TENSOR - 1)
        whole = remote(buffer.at[others], buffer.at[others], i, tensor_peer(1))
        whole.wait_send()
        whole.wait_recv()
        total = buffer[0].astype(F32)
        for k in range(1, TENSOR):
            total = total + buffer[k].astype(F32)
        return total

    projected = sum_over_tensor(partial, proj1, 2, lambda: send_weights(2))
    hidden = (tokens[...].astype(F32) + projected).astype(BF16).astype(F32)

    squares = jnp.sum(hidden * hidden, axis=1, keepdims=True)
    row_of = lax.broadcasted_iota(jnp.int32, (B, HD), 0)
    lane_of = lax.broadcasted_iota(jnp.int32, (B, HD), 1)
    sq_out[...] = jnp.sum(jnp.where(row_of == lane_of, squares, 0.0), axis=0, keepdims=True)
    sq_in[rank] = sq_out[...]

    scaled = (hidden * gains[1]).astype(BF16)
    def rows_of(y2):
        return pl.ds(pl.multiple_of(y2 * ROWS_EACH, ROWS_EACH), ROWS_EACH)

    second_peers = {
        "x": [(0, dy, dz) for dy in (2, 1, 3, 0) for dz in (1, 0) if dy or dz],
        "y": [(dx, 0, dz) for dx in (2, 1, 3, 0) for dz in (1, 0) if dx or dz],
        "z": [(dx, dy, 0) for dx in (2, 1, 3, 0) for dy in (2, 1, 3, 0) if dx or dy],
    }

    def send(i, src, dst, device):
        remote(src, dst, i, device).start()

    def wait_recv(i, like):
        remote(like, like, i, peer(FAR_FIRST[-1])[1]).wait_recv()

    def wait_send(i, like):
        remote(like, like, i, peer(FAR_FIRST[-1])[1]).wait_send()

    step_0, step_1, step_2, step_3, step_4 = (7 + N_CHUNKS * i for i in range(5))
    for p, (kind, _, _) in enumerate(CHUNKS):
        wide_rows[p][:, 0:COLS] = scaled
        for offset in ring[kind]:
            to = wide_rows[p].at[:, pl.ds(step_of(offset) * COLS, COLS)]
            send(step_1 + p, wide_rows[p].at[:, pl.ds(0, COLS)], to, at(*offset)[3])
    for offset in FAR_FIRST:
        remote(sq_out, sq_in.at[rank], 3, peer(offset)[1]).start()
    row_place = {"x": dp, "y": x, "z": dp}
    for p, (kind, _, count) in enumerate(CHUNKS):
        whole = wide_weights[p].at[:, :, pl.ds(0, 128)]
        pltpu.make_async_copy(whole, whole, own_rows_sem.at[p]).wait()
        wait_recv(step_0 + p, wide_weights[p].at[:, :, pl.ds(128, 128 * (WAYS[kind] - 1))])
        wait_recv(step_1 + p, wide_rows[p].at[:, pl.ds(COLS, COLS * (WAYS[kind] - 1))])
        for i in range(NX if kind == "z" else NZ):
            for half in range(2):
                gu_sum[p][i, half] = jnp.dot(
                    wide_rows[p][...], wide_weights[p][i, half], preferred_element_type=F32
                ).astype(BF16)
        for k, offset in enumerate(second_peers[kind]):
            x2, y2, z2, device = at(*offset)
            src = gu_sum[p].at[x2 if kind == "z" else z2, :, rows_of({"x": y2, "y": x2, "z": y2}[kind])]
            send(step_2 + p, src, gu_in2[p].at[k], device)

    wait_all(sq_in.at[rest], sq_in.at[rest], 3)
    total = jnp.sum(sq_in[...], axis=0)
    lane_of = lax.broadcasted_iota(jnp.int32, (ROWS_EACH, HD), 1)
    factors = {}
    for kind in "xy":
        row_of = lax.broadcasted_iota(jnp.int32, (ROWS_EACH, HD), 0) + row_place[kind] * ROWS_EACH
        square = jnp.sum(jnp.where(row_of == lane_of, total, 0.0), axis=1, keepdims=True)
        factors[kind] = lax.rsqrt(square / D + 1e-05)
    factors["z"] = factors["x"]

    def like_3(p):
        return gu_in2[p].at[:, 0]

    def like_4(p):
        if CHUNKS[p][0] == "z":
            return gu_sum[p].at[:, 0]
        return act[p].at[pl.ds(0, 3)]

    def activate(p):
        kind = CHUNKS[p][0]
        wait_recv(step_2 + p, gu_in2[p])
        mine = rows_of(row_place[kind])
        halves = []
        for half in range(2):
            value = gu_sum[p][x if kind == "z" else z, half, mine].astype(F32)
            for k in range(len(second_peers[kind])):
                value = value + gu_in2[p][k, half].astype(F32)
            halves.append(value * factors[kind])
        gate, up = halves
        major = dp if kind == "y" else x
        act[p][major, z, mine] = (gate / (1.0 + jnp.exp(-gate)) * up).astype(BF16)
        block = act[p].at[major, z, mine]
        for offset in second_peers[kind]:
            send(step_3 + p, block, block, at(*offset)[3])

    def pass_on(p):
        kind = CHUNKS[p][0]
        wait_recv(step_3 + p, like_3(p))
        block = {"x": act[p].at[x], "y": act[p].at[dp], "z": act[p].at[:, z]}[kind]
        for offset in ring[kind]:
            send(step_4 + p, block, block, at(*offset)[3])

    def lower(p):
        kind, first, count = CHUNKS[p]
        wait_recv(step_4 + p, like_4(p))
        width = count * 128
        partial = None
        for c in range(SECTIONS):
            start = c * UNITS_EACH + first * 128
            product = jnp.dot(
                act[p][c // NZ, c % NZ], down[start : start + width], preferred_element_type=F32
            )
            partial = product if partial is None else partial + product
        lowered_sum[...] = partial if p == 0 else lowered_sum[...] + partial

    for p in range(N_CHUNKS):
        activate(p)
    for p in range(N_CHUNKS):
        pass_on(p)
    loads[8].wait()
    for p in range(N_CHUNKS):
        lower(p)
    partial = lowered_sum[...]
    lowered = sum_over_tensor(partial, proj2, 6)
    for p, (kind, _, _) in enumerate(CHUNKS):
        wait_send(step_0 + p, wide_weights[p].at[:, :, pl.ds(128, 128 * (WAYS[kind] - 1))])
        wait_send(step_1 + p, wide_rows[p].at[:, pl.ds(COLS, COLS * (WAYS[kind] - 1))])
        wait_send(step_2 + p, gu_in2[p])
        wait_send(step_3 + p, like_3(p))
        wait_send(step_4 + p, like_4(p))
    out_ref[...] = hidden + lowered


def chunk_buffers():
    weights, rows, total, in2, act = [], [], [], [], []
    for kind, first, count in CHUNKS:
        w = count * 128
        blocks, peers = (NX, NX * NY - 1) if kind == "z" else (NZ, NX * NZ - 1)
        weights.append(pltpu.VMEM((blocks, 2, COLS * WAYS[kind], w), BF16))
        rows.append(pltpu.VMEM((B, COLS * WAYS[kind]), BF16))
        total.append(pltpu.VMEM((blocks, 2, B, w), BF16))
        in2.append(pltpu.VMEM((peers, 2, ROWS_EACH, w), BF16))
        act.append(pltpu.VMEM((NX, NZ, B, w), BF16))
    sums = [pltpu.VMEM((B, COLS), F32), pltpu.SemaphoreType.DMA((N_CHUNKS,))]
    return [*weights, *rows, *total, *in2, *act, *sums]


def body(
    tokens,
    attn_gain,
    qkv_weight,
    qkv_order,
    cache_keys,
    cache_values,
    cache_len,
    out_weight,
    ffn_gain,
    gate_up,
    down_weight,
):
    half_dim = HD // 2
    inv_freq = 500000.0 ** (-(2.0 * np.arange(half_dim)) / HD)
    inv_freq = np.concatenate([inv_freq, inv_freq])[None, :].astype(np.float32)
    hbm = pl.BlockSpec(memory_space=pl.ANY)
    out = pl.pallas_call(
        layer_kernel,
        out_shape=jax.ShapeDtypeStruct((B, COLS), F32),
        in_specs=[hbm] * 12,
        out_specs=pl.BlockSpec(memory_space=pltpu.VMEM),
        scratch_shapes=[
            pltpu.SMEM((GROUP,), jnp.int32),
            pltpu.SMEM((SEQS,), jnp.int32),
            pltpu.VMEM((1, HD), F32),
            pltpu.VMEM((B, COLS), BF16),
            pltpu.VMEM((2, 1, COLS), F32),
            pltpu.VMEM(qkv_weight.shape, BF16),
            pltpu.VMEM(cache_keys.shape, BF16),
            pltpu.VMEM(cache_values.shape, BF16),
            pltpu.VMEM(out_weight.shape, BF16),
            pltpu.VMEM(down_weight.shape, BF16),
            pltpu.VMEM((B * SLOT_ROWS, HD), F32),
            pltpu.VMEM((RANKS, SEQS * SLOT_ROWS, HD), BF16),
            pltpu.VMEM((RANKS, SEQS * SLOT_ROWS, HD), BF16),
            pltpu.VMEM((SEQS * LOCAL_HEADS, HD), F32),
            pltpu.VMEM((RANKS, SEQS * LOCAL_HEADS, HD), BF16),
            pltpu.VMEM((B * LOCAL_HEADS, HD), F32),
            pltpu.VMEM((TENSOR, B, COLS), BF16),
            pltpu.VMEM((TENSOR, B, COLS), BF16),
            pltpu.VMEM((1, 128), F32),
            pltpu.VMEM((RANKS, 1, 128), F32),
            *chunk_buffers(),
            pltpu.SemaphoreType.DMA((12,)),
            pltpu.SemaphoreType.DMA((7 + 5 * N_CHUNKS,)),
            pltpu.SemaphoreType.DMA((7 + 5 * N_CHUNKS,)),
        ],
        compiler_params=pltpu.CompilerParams(
            collective_id=0, has_side_effects=True, vmem_limit_bytes=32 * 2**20
        ),
        name="decoder_layer",
    )(
        *(
            pltpu.with_memory_space_constraint(operand, pltpu.HBM)
            for operand in (
                qkv_order,
                cache_len,
                jnp.asarray(inv_freq),
                tokens,
                attn_gain.reshape(1, COLS),
                ffn_gain.reshape(1, COLS),
                qkv_weight,
                cache_keys,
                cache_values,
                out_weight,
                gate_up,
                down_weight,
            )
        )
    )
    return out.astype(BF16)


def solution(mesh):
    rows = P(None, ("section", "dp"))
    return jax.shard_map(
        body,
        mesh=mesh,
        in_specs=(
            rows,
            P(("section", "dp")),
            P(("section", "dp"), "tensor"),
            P(),
            P(("section", "dp"), "tensor", None, None),
            P(("section", "dp"), "tensor", None, None),
            P(("section", "dp")),
            P("tensor", ("section", "dp")),
            P(("section", "dp")),
            P(None, ("section", "dp"), "tensor"),
            P("tensor", ("section", "dp")),
        ),
        out_specs=rows,
        check_vma=False,
    )
```

```python
import jax
import jax.numpy as jnp
import numpy as np
from jax import lax
from jax.experimental import pallas as pl
from jax.experimental.pallas import tpu as pltpu
from jax.sharding import PartitionSpec as P

D = 4096
HEADS = 64
KV_HEADS = 8
HD = 128
FF = 28672
LEN = 4096
GROUP = 10
B = 64
RANKS = 32
TENSOR = 4
DP = 4
SEQS = B // RANKS
LOCAL_GROUPS = KV_HEADS // TENSOR
PER_GROUP = HEADS // KV_HEADS
COLS = D // RANKS
SLOT_ROWS = 24
LOCAL_HEADS = HEADS // TENSOR
UNITS = FF // TENSOR
SECTIONS = 8
NX, NY, NZ = 4, 4, 2
ROWS_EACH = B // NY
UNITS_EACH = UNITS // SECTIONS
FAR_FIRST = sorted(
    [(dx, dy, dz) for dx in range(NX) for dy in range(NY) for dz in range(NZ) if dx or dy or dz],
    key=lambda o: -(min(o[0], NX - o[0]) + min(o[1], NY - o[1]) + 2 * o[2]),
)
CHUNKS = (("x", 0, 2), ("y", 2, 2), ("z", 4, 2))
LAST = 6
N_CHUNKS = len(CHUNKS)
WAYS = {"x": NX, "y": NY, "z": NZ}
BATCHES = {"x": (4, 8, 0), "y": (4, 8, 0), "z": (3, 5, 0)}
MESH = pl.DeviceIdType.MESH
F32 = jnp.float32
BF16 = jnp.bfloat16


def layer_kernel(
    order_hbm,
    len_hbm,
    freq_hbm,
    tokens_hbm,
    gain1_hbm,
    gain2_hbm,
    qkv_hbm,
    keys_hbm,
    values_hbm,
    outw_hbm,
    gate_up_hbm,
    down_hbm,
    out_ref,
    order_ref,
    len_ref,
    freq,
    tokens,
    gains,
    qkvw,
    keys,
    values,
    outw,
    down,
    joined32,
    joined_out,
    joined_in,
    att_out,
    att_in,
    att32,
    proj1,
    proj2,
    sq_out,
    sq_in,
    *rest_refs,
):
    wide_weights, wide_rows, gu_sum, gu_in2, act = (rest_refs[N_CHUNKS * i : N_CHUNKS * (i + 1)] for i in range(5))
    last_weights, last_sum, last_in, last_act = rest_refs[5 * N_CHUNKS : 5 * N_CHUNKS + 4]
    lowered_sum, own_rows_sem, load_sem, send_sem, recv_sem = rest_refs[5 * N_CHUNKS + 4 :]
    section = lax.axis_index("section")
    x = section // NZ
    z = lax.rem(section, NZ)
    dp = lax.axis_index("dp")
    tensor = lax.axis_index("tensor")
    rank = section * DP + dp

    def load(i, src, dst):
        return pltpu.make_async_copy(src, dst, load_sem.at[i])

    loads = {
        0: load(0, tokens_hbm, tokens),
        1: load(1, gain1_hbm, gains.at[0]),
        2: load(2, qkv_hbm, qkvw),
        3: load(3, freq_hbm, freq),
        9: load(9, gain2_hbm, gains.at[1]),
        10: load(10, order_hbm, order_ref),
        11: load(11, len_hbm, len_ref),
        4: load(4, keys_hbm, keys),
        5: load(5, values_hbm, values),
        6: load(6, outw_hbm, outw),
        8: load(8, down_hbm, down),
    }
    def at(dx, dy, dz):
        x2, y2, z2 = lax.rem(x + dx, NX), lax.rem(dp + dy, NY), lax.rem(z + dz, NZ)
        return x2, y2, z2, {"section": x2 * NZ + z2, "dp": y2}

    def peer(offset):
        x2, y2, z2, device = at(*offset)
        return (x2 * NZ + z2) * DP + y2, device

    def tensor_peer(k):
        return {"tensor": lax.rem(tensor + k, TENSOR)}

    barrier = pltpu.get_barrier_semaphore()

    for offset in FAR_FIRST:
        pl.semaphore_signal(barrier, inc=1, device_id=peer(offset)[1], device_id_type=MESH)
    for k in range(1, TENSOR):
        pl.semaphore_signal(barrier, inc=1, device_id=tensor_peer(k), device_id_type=MESH)

    for copy in loads.values():
        copy.start()

    loads[0].wait()
    loads[1].wait()
    wide = tokens[...].astype(F32)
    squares = jnp.sum(wide * wide, axis=1, keepdims=True)
    left = jnp.broadcast_to(squares, (B, HD))
    for i in range(3):
        part = left.astype(BF16).astype(F32)
        joined32[pl.Slice(20 + i, B, SLOT_ROWS)] = part
        left = left - part
    joined32[pl.Slice(23, B, SLOT_ROWS)] = jnp.zeros((B, HD), F32)
    scaled = (wide * gains[0]).astype(BF16)
    loads[2].wait()
    for j in range(LOCAL_GROUPS * GROUP // 2):
        product = jnp.dot(scaled, qkvw[:, j * 256 : j * 256 + 256], preferred_element_type=F32)
        joined32[pl.Slice(2 * j, B, SLOT_ROWS)] = product[:, :HD]
        joined32[pl.Slice(2 * j + 1, B, SLOT_ROWS)] = product[:, HD:]

    def pack(i, carry):
        joined_out[i] = joined32[pl.ds(i * SEQS * SLOT_ROWS, SEQS * SLOT_ROWS)].astype(BF16)
        return carry

    lax.fori_loop(0, RANKS, pack, 0)
    for i in (3, 9, 10, 11):
        loads[i].wait()
    low = lax.broadcasted_iota(jnp.int32, (1, HD), 1) < HD // 2
    cosines, sines = [], []
    for b in range(SEQS):
        angle = freq[...] * len_ref[b].astype(F32)
        cosines.append(jnp.cos(angle))
        sine = jnp.sin(angle)
        sines.append(jnp.where(low, -sine, sine))
    joined_in[rank] = joined_out[rank]

    pl.semaphore_wait(barrier, RANKS - 1 + TENSOR - 1)

    def remote(src, dst, i, device):
        return pltpu.make_async_remote_copy(
            src_ref=src,
            dst_ref=dst,
            send_sem=send_sem.at[i],
            recv_sem=recv_sem.at[i],
            device_id=device,
            device_id_type=MESH,
        )

    ring = {
        "x": [(2, 0, 0), (1, 0, 0), (3, 0, 0)],
        "y": [(0, 2, 0), (0, 1, 0), (0, 3, 0)],
        "z": [(0, 0, 1)],
    }

    def block_start(p, major, minor):
        return pl.multiple_of((major * NZ + minor) * UNITS_EACH + CHUNKS[p][1] * 128, 128)

    def weight_piece(p, to, i, half):
        kind, _, count = CHUNKS[p]
        start = block_start(p, i, to) if kind == "z" else block_start(p, to, i)
        return gate_up_hbm.at[half, :, pl.ds(start, count * 128)]

    def step_of(offset):
        return max(offset)

    place = {"x": x, "y": dp, "z": z}
    pieces = {}
    for p, (kind, _, _) in enumerate(CHUNKS):
        pieces[p] = [
            (offset, i, half) for i in range(NX if kind == "z" else NZ) for half in range(2) for offset in ring[kind]
        ]
        for i in range(NX if kind == "z" else NZ):
            for half in range(2):
                pltpu.make_async_copy(
                    weight_piece(p, place[kind], i, half), wide_weights[p].at[i, half, pl.ds(0, 128)], own_rows_sem.at[p]
                ).start()

    for c in range(SECTIONS):
        src = gate_up_hbm.at[:, :, pl.ds(c * UNITS_EACH + LAST * 128, 128)]
        pltpu.make_async_copy(src, last_weights.at[c], own_rows_sem.at[N_CHUNKS]).start()

    def send_weights(batch):
        for p, (kind, _, _) in enumerate(CHUNKS):
            first = sum(BATCHES[kind][:batch])
            for offset, i, half in pieces[p][first : first + BATCHES[kind][batch]]:
                to = at(*offset)
                dst = wide_weights[p].at[i, half, pl.ds(step_of(offset) * 128, 128)]
                remote(weight_piece(p, to["xyz".index(kind)], i, half), dst, 7 + p, to[3]).start()

    for offset in FAR_FIRST:
        other, device = peer(offset)
        remote(joined_out.at[other], joined_in.at[rank], 0, device).start()
    send_weights(0)

    def wait_all(src, dst, i):
        whole = remote(src, dst, i, peer(FAR_FIRST[-1])[1])
        whole.wait_send()
        whole.wait_recv()

    rest = pl.ds(0, RANKS - 1)
    wait_all(joined_out.at[rest], joined_in.at[rest], 0)

    joined = joined_in[0].astype(F32)
    for i in range(1, RANKS):
        joined = joined + joined_in[i].astype(F32)

    loads[4].wait()
    loads[5].wait()
    inv_scale = HD**-0.5
    position = lax.broadcasted_iota(jnp.int32, (PER_GROUP, LEN), 1)
    logical_row = lax.broadcasted_iota(jnp.int32, (16, HD), 0)
    for b in range(SEQS):
        base = b * SLOT_ROWS
        total = joined[base + 20 : base + 21] + joined[base + 21 : base + 22] + joined[base + 22 : base + 23]
        factor = lax.rsqrt(total / D + 1e-05)
        for g in range(LOCAL_GROUPS):
            logical = jnp.zeros((16, HD), F32)
            for j in range(GROUP):
                row = joined[base + g * GROUP + j : base + g * GROUP + j + 1]
                logical = jnp.where(logical_row == order_ref[j], row, logical)
            logical = logical * factor
            rotated = logical * cosines[b] + pltpu.roll(logical, HD // 2, 1) * sines[b]
            rotated = rotated.astype(BF16)
            queries = rotated[0:PER_GROUP]
            new_key = rotated.astype(F32)[PER_GROUP : PER_GROUP + 1]
            new_value = logical[PER_GROUP + 1 : PER_GROUP + 2].astype(BF16).astype(F32)
            own = jnp.sum(queries.astype(F32) * new_key, axis=1, keepdims=True)
            scores = lax.dot_general(
                queries, keys[b, g], (((1,), (1,)), ((), ())), preferred_element_type=F32
            )
            masked = jnp.where(position < len_ref[b], scores, -jnp.inf)
            peak = jnp.maximum(jnp.max(masked, axis=1, keepdims=True), own)
            weights = jnp.exp((masked - peak) * inv_scale)
            own_weight = jnp.exp((own - peak) * inv_scale)
            denom = jnp.sum(weights, axis=1, keepdims=True) + own_weight
            mixed = jnp.dot(weights.astype(BF16), values[b, g], preferred_element_type=F32)
            mixed = mixed + own_weight.astype(BF16).astype(F32) * new_value
            att_out[pl.ds((b * LOCAL_GROUPS + g) * PER_GROUP, PER_GROUP)] = mixed / denom

    att_in[rank] = att_out[...].astype(BF16)

    for offset in FAR_FIRST:
        remote(att_in.at[rank], att_in.at[rank], 1, peer(offset)[1]).start()
    send_weights(1)
    wait_all(att_in.at[rest], att_in.at[rest], 1)

    def widen(i, carry):
        att32[pl.ds(i * SEQS * LOCAL_HEADS, SEQS * LOCAL_HEADS)] = att_in[i].astype(F32)
        return carry

    lax.fori_loop(0, RANKS, widen, 0)
    loads[6].wait()
    attended = jnp.concatenate([att32[pl.Slice(h, B, LOCAL_HEADS)].astype(BF16) for h in range(LOCAL_HEADS)], axis=1)
    partial = jnp.dot(attended, outw[...], preferred_element_type=F32)

    def sum_over_tensor(value, buffer, i, then=lambda: None):
        buffer[tensor] = value.astype(BF16)
        for k in range(1, TENSOR):
            remote(buffer.at[tensor], buffer.at[tensor], i, tensor_peer(k)).start()
        then()
        others = pl.ds(0, TENSOR - 1)
        whole = remote(buffer.at[others], buffer.at[others], i, tensor_peer(1))
        whole.wait_send()
        whole.wait_recv()
        total = buffer[0].astype(F32)
        for k in range(1, TENSOR):
            total = total + buffer[k].astype(F32)
        return total

    projected = sum_over_tensor(partial, proj1, 2, lambda: send_weights(2))
    hidden = (tokens[...].astype(F32) + projected).astype(BF16).astype(F32)

    squares = jnp.sum(hidden * hidden, axis=1, keepdims=True)
    row_of = lax.broadcasted_iota(jnp.int32, (B, HD), 0)
    lane_of = lax.broadcasted_iota(jnp.int32, (B, HD), 1)
    sq_out[...] = jnp.sum(jnp.where(row_of == lane_of, squares, 0.0), axis=0, keepdims=True)
    sq_in[rank] = sq_out[...]

    scaled = (hidden * gains[1]).astype(BF16)
    def rows_of(y2):
        return pl.ds(pl.multiple_of(y2 * ROWS_EACH, ROWS_EACH), ROWS_EACH)

    second_peers = {
        "x": [(0, dy, dz) for dy in (2, 1, 3, 0) for dz in (1, 0) if dy or dz],
        "y": [(dx, 0, dz) for dx in (2, 1, 3, 0) for dz in (1, 0) if dx or dz],
        "z": [(dx, dy, 0) for dx in (2, 1, 3, 0) for dy in (2, 1, 3, 0) if dx or dy],
    }

    def send(i, src, dst, device):
        remote(src, dst, i, device).start()

    def wait_recv(i, like):
        remote(like, like, i, peer(FAR_FIRST[-1])[1]).wait_recv()

    def wait_send(i, like):
        remote(like, like, i, peer(FAR_FIRST[-1])[1]).wait_send()

    step_0, step_1, step_2, step_3, step_4 = (7 + N_CHUNKS * i for i in range(5))
    for p, (kind, _, _) in enumerate(CHUNKS):
        wide_rows[p][:, 0:COLS] = scaled
        for offset in ring[kind]:
            to = wide_rows[p].at[:, pl.ds(step_of(offset) * COLS, COLS)]
            send(step_1 + p, wide_rows[p].at[:, pl.ds(0, COLS)], to, at(*offset)[3])
    pltpu.make_async_copy(last_weights, last_weights, own_rows_sem.at[N_CHUNKS]).wait()
    for c in range(SECTIONS):
        for half in range(2):
            product = jnp.dot(scaled, last_weights[c, half], preferred_element_type=F32)
            last_sum[c, half] = product.astype(BF16)
    for k, offset in enumerate(FAR_FIRST):
        x2, y2, z2, device = at(*offset)
        send(4, last_sum.at[x2 * NZ + z2, :, rows_of(y2)], last_in.at[k], device)
    for offset in FAR_FIRST:
        remote(sq_out, sq_in.at[rank], 3, peer(offset)[1]).start()
    row_place = {"x": dp, "y": x, "z": dp}
    for p, (kind, _, count) in enumerate(CHUNKS):
        whole = wide_weights[p].at[:, :, pl.ds(0, 128)]
        pltpu.make_async_copy(whole, whole, own_rows_sem.at[p]).wait()
        wait_recv(step_0 + p, wide_weights[p].at[:, :, pl.ds(128, 128 * (WAYS[kind] - 1))])
        wait_recv(step_1 + p, wide_rows[p].at[:, pl.ds(COLS, COLS * (WAYS[kind] - 1))])
        for i in range(NX if kind == "z" else NZ):
            for half in range(2):
                gu_sum[p][i, half] = jnp.dot(
                    wide_rows[p][...], wide_weights[p][i, half], preferred_element_type=F32
                ).astype(BF16)
        for k, offset in enumerate(second_peers[kind]):
            x2, y2, z2, device = at(*offset)
            src = gu_sum[p].at[x2 if kind == "z" else z2, :, rows_of({"x": y2, "y": x2, "z": y2}[kind])]
            send(step_2 + p, src, gu_in2[p].at[k], device)

    wait_all(sq_in.at[rest], sq_in.at[rest], 3)
    total = jnp.sum(sq_in[...], axis=0)
    lane_of = lax.broadcasted_iota(jnp.int32, (ROWS_EACH, HD), 1)
    factors = {}
    for kind in "xy":
        row_of = lax.broadcasted_iota(jnp.int32, (ROWS_EACH, HD), 0) + row_place[kind] * ROWS_EACH
        square = jnp.sum(jnp.where(row_of == lane_of, total, 0.0), axis=1, keepdims=True)
        factors[kind] = lax.rsqrt(square / D + 1e-05)
    factors["z"] = factors["x"]

    def activate_last():
        wait_recv(4, last_in)
        mine = rows_of(dp)
        halves = []
        for half in range(2):
            value = last_sum[section, half, mine].astype(F32)
            for k in range(RANKS - 1):
                value = value + last_in[k, half].astype(F32)
            halves.append(value * factors["x"])
        gate, up = halves
        last_act[section, mine] = (gate / (1.0 + jnp.exp(-gate)) * up).astype(BF16)
        block = last_act.at[section, mine]
        for offset in FAR_FIRST:
            send(5, block, block, at(*offset)[3])

    def lower_last():
        wait_recv(5, last_in.at[:, 0])
        partial = jnp.zeros((B, COLS), F32)
        for c in range(SECTIONS):
            start = c * UNITS_EACH + LAST * 128
            partial = partial + jnp.dot(
                last_act[c], down[start : start + 128], preferred_element_type=F32
            )
        lowered_sum[...] = partial

    def like_3(p):
        return gu_in2[p].at[:, 0]

    def like_4(p):
        if CHUNKS[p][0] == "z":
            return gu_sum[p].at[:, 0]
        return act[p].at[pl.ds(0, 3)]

    def activate(p):
        kind = CHUNKS[p][0]
        wait_recv(step_2 + p, gu_in2[p])
        mine = rows_of(row_place[kind])
        halves = []
        for half in range(2):
            value = gu_sum[p][x if kind == "z" else z, half, mine].astype(F32)
            for k in range(len(second_peers[kind])):
                value = value + gu_in2[p][k, half].astype(F32)
            halves.append(value * factors[kind])
        gate, up = halves
        major = dp if kind == "y" else x
        act[p][major, z, mine] = (gate / (1.0 + jnp.exp(-gate)) * up).astype(BF16)
        block = act[p].at[major, z, mine]
        for offset in second_peers[kind]:
            send(step_3 + p, block, block, at(*offset)[3])

    def pass_on(p):
        kind = CHUNKS[p][0]
        wait_recv(step_3 + p, like_3(p))
        block = {"x": act[p].at[x], "y": act[p].at[dp], "z": act[p].at[:, z]}[kind]
        for offset in ring[kind]:
            send(step_4 + p, block, block, at(*offset)[3])

    def lower(p):
        kind, first, count = CHUNKS[p]
        wait_recv(step_4 + p, like_4(p))
        width = count * 128
        partial = None
        for c in range(SECTIONS):
            start = c * UNITS_EACH + first * 128
            product = jnp.dot(
                act[p][c // NZ, c % NZ], down[start : start + width], preferred_element_type=F32
            )
            partial = product if partial is None else partial + product
        lowered_sum[...] = lowered_sum[...] + partial

    for p in range(N_CHUNKS):
        activate(p)
    activate_last()
    for p in range(N_CHUNKS):
        pass_on(p)
    loads[8].wait()
    lower_last()
    for p in range(N_CHUNKS):
        lower(p)
    partial = lowered_sum[...]
    lowered = sum_over_tensor(partial, proj2, 6)
    wait_send(4, last_in)
    wait_send(5, last_in.at[:, 0])
    for p, (kind, _, _) in enumerate(CHUNKS):
        wait_send(step_0 + p, wide_weights[p].at[:, :, pl.ds(128, 128 * (WAYS[kind] - 1))])
        wait_send(step_1 + p, wide_rows[p].at[:, pl.ds(COLS, COLS * (WAYS[kind] - 1))])
        wait_send(step_2 + p, gu_in2[p])
        wait_send(step_3 + p, like_3(p))
        wait_send(step_4 + p, like_4(p))
    out_ref[...] = hidden + lowered


def chunk_buffers():
    weights, rows, total, in2, act = [], [], [], [], []
    for kind, first, count in CHUNKS:
        w = count * 128
        blocks, peers = (NX, NX * NY - 1) if kind == "z" else (NZ, NX * NZ - 1)
        weights.append(pltpu.VMEM((blocks, 2, COLS * WAYS[kind], w), BF16))
        rows.append(pltpu.VMEM((B, COLS * WAYS[kind]), BF16))
        total.append(pltpu.VMEM((blocks, 2, B, w), BF16))
        in2.append(pltpu.VMEM((peers, 2, ROWS_EACH, w), BF16))
        act.append(pltpu.VMEM((NX, NZ, B, w), BF16))
    sums = [
        pltpu.VMEM((SECTIONS, 2, COLS, 128), BF16),
        pltpu.VMEM((SECTIONS, 2, B, 128), BF16),
        pltpu.VMEM((RANKS - 1, 2, ROWS_EACH, 128), BF16),
        pltpu.VMEM((SECTIONS, B, 128), BF16),
        pltpu.VMEM((B, COLS), F32),
        pltpu.SemaphoreType.DMA((N_CHUNKS + 1,)),
    ]
    return [*weights, *rows, *total, *in2, *act, *sums]


def body(
    tokens,
    attn_gain,
    qkv_weight,
    qkv_order,
    cache_keys,
    cache_values,
    cache_len,
    out_weight,
    ffn_gain,
    gate_up,
    down_weight,
):
    half_dim = HD // 2
    inv_freq = 500000.0 ** (-(2.0 * np.arange(half_dim)) / HD)
    inv_freq = np.concatenate([inv_freq, inv_freq])[None, :].astype(np.float32)
    hbm = pl.BlockSpec(memory_space=pl.ANY)
    out = pl.pallas_call(
        layer_kernel,
        out_shape=jax.ShapeDtypeStruct((B, COLS), F32),
        in_specs=[hbm] * 12,
        out_specs=pl.BlockSpec(memory_space=pltpu.VMEM),
        scratch_shapes=[
            pltpu.SMEM((GROUP,), jnp.int32),
            pltpu.SMEM((SEQS,), jnp.int32),
            pltpu.VMEM((1, HD), F32),
            pltpu.VMEM((B, COLS), BF16),
            pltpu.VMEM((2, 1, COLS), F32),
            pltpu.VMEM(qkv_weight.shape, BF16),
            pltpu.VMEM(cache_keys.shape, BF16),
            pltpu.VMEM(cache_values.shape, BF16),
            pltpu.VMEM(out_weight.shape, BF16),
            pltpu.VMEM(down_weight.shape, BF16),
            pltpu.VMEM((B * SLOT_ROWS, HD), F32),
            pltpu.VMEM((RANKS, SEQS * SLOT_ROWS, HD), BF16),
            pltpu.VMEM((RANKS, SEQS * SLOT_ROWS, HD), BF16),
            pltpu.VMEM((SEQS * LOCAL_HEADS, HD), F32),
            pltpu.VMEM((RANKS, SEQS * LOCAL_HEADS, HD), BF16),
            pltpu.VMEM((B * LOCAL_HEADS, HD), F32),
            pltpu.VMEM((TENSOR, B, COLS), BF16),
            pltpu.VMEM((TENSOR, B, COLS), BF16),
            pltpu.VMEM((1, 128), F32),
            pltpu.VMEM((RANKS, 1, 128), F32),
            *chunk_buffers(),
            pltpu.SemaphoreType.DMA((12,)),
            pltpu.SemaphoreType.DMA((7 + 5 * N_CHUNKS,)),
            pltpu.SemaphoreType.DMA((7 + 5 * N_CHUNKS,)),
        ],
        compiler_params=pltpu.CompilerParams(
            collective_id=0, has_side_effects=True, vmem_limit_bytes=32 * 2**20
        ),
        name="decoder_layer",
    )(
        *(
            pltpu.with_memory_space_constraint(operand, pltpu.HBM)
            for operand in (
                qkv_order,
                cache_len,
                jnp.asarray(inv_freq),
                tokens,
                attn_gain.reshape(1, COLS),
                ffn_gain.reshape(1, COLS),
                qkv_weight,
                cache_keys,
                cache_values,
                out_weight,
                gate_up,
                down_weight,
            )
        )
    )
    return out.astype(BF16)


def solution(mesh):
    rows = P(None, ("section", "dp"))
    return jax.shard_map(
        body,
        mesh=mesh,
        in_specs=(
            rows,
            P(("section", "dp")),
            P(("section", "dp"), "tensor"),
            P(),
            P(("section", "dp"), "tensor", None, None),
            P(("section", "dp"), "tensor", None, None),
            P(("section", "dp")),
            P("tensor", ("section", "dp")),
            P(("section", "dp")),
            P(None, ("section", "dp"), "tensor"),
            P("tensor", ("section", "dp")),
        ),
        out_specs=rows,
        check_vma=False,
    )
```

```python
import jax
import jax.numpy as jnp
import numpy as np
from jax import lax
from jax.experimental import pallas as pl
from jax.experimental.pallas import tpu as pltpu
from jax.sharding import PartitionSpec as P

D = 4096
HEADS = 64
KV_HEADS = 8
HD = 128
FF = 28672
LEN = 4096
GROUP = 10
B = 64
RANKS = 32
TENSOR = 4
DP = 4
SEQS = B // RANKS
LOCAL_GROUPS = KV_HEADS // TENSOR
PER_GROUP = HEADS // KV_HEADS
COLS = D // RANKS
SLOT_ROWS = 24
LOCAL_HEADS = HEADS // TENSOR
UNITS = FF // TENSOR
SECTIONS = 8
NX, NY, NZ = 4, 4, 2
ROWS_EACH = B // NY
UNITS_EACH = UNITS // SECTIONS
FAR_FIRST = sorted(
    [(dx, dy, dz) for dx in range(NX) for dy in range(NY) for dz in range(NZ) if dx or dy or dz],
    key=lambda o: -(min(o[0], NX - o[0]) + min(o[1], NY - o[1]) + 2 * o[2]),
)
CHUNKS = (("x", 0, 2), ("y", 2, 2), ("z", 4, 2))
LAST = 6
N_CHUNKS = len(CHUNKS)
WAYS = {"x": NX, "y": NY, "z": NZ}
BATCHES = {"x": (4,7,1), "y": (4,7,1), "z": (4,4,0)}
MESH = pl.DeviceIdType.MESH
F32 = jnp.float32
BF16 = jnp.bfloat16


def layer_kernel(
    order_hbm,
    len_hbm,
    freq_hbm,
    tokens_hbm,
    gain1_hbm,
    gain2_hbm,
    qkv_hbm,
    keys_hbm,
    values_hbm,
    outw_hbm,
    gate_up_hbm,
    down_hbm,
    out_ref,
    order_ref,
    len_ref,
    freq,
    tokens,
    gains,
    qkvw,
    keys,
    values,
    outw,
    down,
    joined32,
    joined_out,
    joined_in,
    att_out,
    att_in,
    att32,
    proj1,
    proj2,
    sq_out,
    sq_in,
    *rest_refs,
):
    wide_weights, wide_rows, gu_sum, gu_in2, act = (rest_refs[N_CHUNKS * i : N_CHUNKS * (i + 1)] for i in range(5))
    last_weights, last_sum, last_in, last_act = rest_refs[5 * N_CHUNKS : 5 * N_CHUNKS + 4]
    lowered_sum, own_rows_sem, load_sem, send_sem, recv_sem = rest_refs[5 * N_CHUNKS + 4 :]
    section = lax.axis_index("section")
    x = section // NZ
    z = lax.rem(section, NZ)
    dp = lax.axis_index("dp")
    tensor = lax.axis_index("tensor")
    rank = section * DP + dp

    def load(i, src, dst):
        return pltpu.make_async_copy(src, dst, load_sem.at[i])

    loads = {
        0: load(0, tokens_hbm, tokens),
        1: load(1, gain1_hbm, gains.at[0]),
        2: load(2, qkv_hbm, qkvw),
        3: load(3, freq_hbm, freq),
        9: load(9, gain2_hbm, gains.at[1]),
        10: load(10, order_hbm, order_ref),
        11: load(11, len_hbm, len_ref),
        4: load(4, keys_hbm, keys),
        5: load(5, values_hbm, values),
        6: load(6, outw_hbm, outw),
        8: load(8, down_hbm, down),
    }
    def at(dx, dy, dz):
        x2, y2, z2 = lax.rem(x + dx, NX), lax.rem(dp + dy, NY), lax.rem(z + dz, NZ)
        return x2, y2, z2, {"section": x2 * NZ + z2, "dp": y2}

    def peer(offset):
        x2, y2, z2, device = at(*offset)
        return (x2 * NZ + z2) * DP + y2, device

    def tensor_peer(k):
        return {"tensor": lax.rem(tensor + k, TENSOR)}

    barrier = pltpu.get_barrier_semaphore()

    for offset in FAR_FIRST:
        pl.semaphore_signal(barrier, inc=1, device_id=peer(offset)[1], device_id_type=MESH)
    for k in range(1, TENSOR):
        pl.semaphore_signal(barrier, inc=1, device_id=tensor_peer(k), device_id_type=MESH)

    for copy in loads.values():
        copy.start()

    loads[0].wait()
    loads[1].wait()
    wide = tokens[...].astype(F32)
    squares = jnp.sum(wide * wide, axis=1, keepdims=True)
    left = jnp.broadcast_to(squares, (B, HD))
    for i in range(3):
        part = left.astype(BF16).astype(F32)
        joined32[pl.Slice(20 + i, B, SLOT_ROWS)] = part
        left = left - part
    joined32[pl.Slice(23, B, SLOT_ROWS)] = jnp.zeros((B, HD), F32)
    scaled = (wide * gains[0]).astype(BF16)
    loads[2].wait()
    for j in range(LOCAL_GROUPS * GROUP // 2):
        product = jnp.dot(scaled, qkvw[:, j * 256 : j * 256 + 256], preferred_element_type=F32)
        joined32[pl.Slice(2 * j, B, SLOT_ROWS)] = product[:, :HD]
        joined32[pl.Slice(2 * j + 1, B, SLOT_ROWS)] = product[:, HD:]

    def pack(i, carry):
        joined_out[i] = joined32[pl.ds(i * SEQS * SLOT_ROWS, SEQS * SLOT_ROWS)].astype(BF16)
        return carry

    lax.fori_loop(0, RANKS, pack, 0)
    for i in (3, 9, 10, 11):
        loads[i].wait()
    low = lax.broadcasted_iota(jnp.int32, (1, HD), 1) < HD // 2
    cosines, sines = [], []
    for b in range(SEQS):
        angle = freq[...] * len_ref[b].astype(F32)
        cosines.append(jnp.cos(angle))
        sine = jnp.sin(angle)
        sines.append(jnp.where(low, -sine, sine))
    joined_in[rank] = joined_out[rank]

    pl.semaphore_wait(barrier, RANKS - 1 + TENSOR - 1)

    def remote(src, dst, i, device):
        return pltpu.make_async_remote_copy(
            src_ref=src,
            dst_ref=dst,
            send_sem=send_sem.at[i],
            recv_sem=recv_sem.at[i],
            device_id=device,
            device_id_type=MESH,
        )

    ring = {
        "x": [(2, 0, 0), (1, 0, 0), (3, 0, 0)],
        "y": [(0, 2, 0), (0, 1, 0), (0, 3, 0)],
        "z": [(0, 0, 1)],
    }

    def block_start(p, major, minor):
        return pl.multiple_of((major * NZ + minor) * UNITS_EACH + CHUNKS[p][1] * 128, 128)

    def weight_piece(p, to, i, half):
        kind, _, count = CHUNKS[p]
        start = block_start(p, i, to) if kind == "z" else block_start(p, to, i)
        return gate_up_hbm.at[half, :, pl.ds(start, count * 128)]

    def step_of(offset):
        return max(offset)

    place = {"x": x, "y": dp, "z": z}
    pieces = {}
    for p, (kind, _, _) in enumerate(CHUNKS):
        pieces[p] = [
            (offset, i, half) for i in range(NX if kind == "z" else NZ) for half in range(2) for offset in ring[kind]
        ]
        for i in range(NX if kind == "z" else NZ):
            for half in range(2):
                pltpu.make_async_copy(
                    weight_piece(p, place[kind], i, half), wide_weights[p].at[i, half, pl.ds(0, 128)], own_rows_sem.at[p]
                ).start()

    for c in range(SECTIONS):
        src = gate_up_hbm.at[:, :, pl.ds(c * UNITS_EACH + LAST * 128, 128)]
        pltpu.make_async_copy(src, last_weights.at[c], own_rows_sem.at[N_CHUNKS]).start()

    def send_weights(batch):
        for p, (kind, _, _) in enumerate(CHUNKS):
            first = sum(BATCHES[kind][:batch])
            for offset, i, half in pieces[p][first : first + BATCHES[kind][batch]]:
                to = at(*offset)
                dst = wide_weights[p].at[i, half, pl.ds(step_of(offset) * 128, 128)]
                remote(weight_piece(p, to["xyz".index(kind)], i, half), dst, 7 + p, to[3]).start()

    for offset in FAR_FIRST:
        other, device = peer(offset)
        remote(joined_out.at[other], joined_in.at[rank], 0, device).start()
    send_weights(0)

    def wait_all(src, dst, i):
        whole = remote(src, dst, i, peer(FAR_FIRST[-1])[1])
        whole.wait_send()
        whole.wait_recv()

    rest = pl.ds(0, RANKS - 1)
    wait_all(joined_out.at[rest], joined_in.at[rest], 0)

    joined = joined_in[0].astype(F32)
    for i in range(1, RANKS):
        joined = joined + joined_in[i].astype(F32)

    loads[4].wait()
    loads[5].wait()
    inv_scale = HD**-0.5
    position = lax.broadcasted_iota(jnp.int32, (PER_GROUP, LEN), 1)
    logical_row = lax.broadcasted_iota(jnp.int32, (16, HD), 0)
    for b in range(SEQS):
        base = b * SLOT_ROWS
        total = joined[base + 20 : base + 21] + joined[base + 21 : base + 22] + joined[base + 22 : base + 23]
        factor = lax.rsqrt(total / D + 1e-05)
        for g in range(LOCAL_GROUPS):
            logical = jnp.zeros((16, HD), F32)
            for j in range(GROUP):
                row = joined[base + g * GROUP + j : base + g * GROUP + j + 1]
                logical = jnp.where(logical_row == order_ref[j], row, logical)
            logical = logical * factor
            rotated = logical * cosines[b] + pltpu.roll(logical, HD // 2, 1) * sines[b]
            rotated = rotated.astype(BF16)
            queries = rotated[0:PER_GROUP]
            new_key = rotated.astype(F32)[PER_GROUP : PER_GROUP + 1]
            new_value = logical[PER_GROUP + 1 : PER_GROUP + 2].astype(BF16).astype(F32)
            own = jnp.sum(queries.astype(F32) * new_key, axis=1, keepdims=True)
            scores = lax.dot_general(
                queries, keys[b, g], (((1,), (1,)), ((), ())), preferred_element_type=F32
            )
            masked = jnp.where(position < len_ref[b], scores, -jnp.inf)
            peak = jnp.maximum(jnp.max(masked, axis=1, keepdims=True), own)
            weights = jnp.exp((masked - peak) * inv_scale)
            own_weight = jnp.exp((own - peak) * inv_scale)
            denom = jnp.sum(weights, axis=1, keepdims=True) + own_weight
            mixed = jnp.dot(weights.astype(BF16), values[b, g], preferred_element_type=F32)
            mixed = mixed + own_weight.astype(BF16).astype(F32) * new_value
            att_out[pl.ds((b * LOCAL_GROUPS + g) * PER_GROUP, PER_GROUP)] = mixed / denom

    att_in[rank] = att_out[...].astype(BF16)

    for offset in FAR_FIRST:
        remote(att_in.at[rank], att_in.at[rank], 1, peer(offset)[1]).start()
    send_weights(1)
    wait_all(att_in.at[rest], att_in.at[rest], 1)

    def widen(i, carry):
        att32[pl.ds(i * SEQS * LOCAL_HEADS, SEQS * LOCAL_HEADS)] = att_in[i].astype(F32)
        return carry

    lax.fori_loop(0, RANKS, widen, 0, unroll=True)
    loads[6].wait()
    attended = jnp.concatenate([att32[pl.Slice(h, B, LOCAL_HEADS)].astype(BF16) for h in range(LOCAL_HEADS)], axis=1)
    partial = jnp.dot(attended, outw[...], preferred_element_type=F32)

    def sum_over_tensor(value, buffer, i, then=lambda: None):
        buffer[tensor] = value.astype(BF16)
        for k in range(1, TENSOR):
            remote(buffer.at[tensor], buffer.at[tensor], i, tensor_peer(k)).start()
        then()
        others = pl.ds(0, TENSOR - 1)
        whole = remote(buffer.at[others], buffer.at[others], i, tensor_peer(1))
        whole.wait_send()
        whole.wait_recv()
        total = buffer[0].astype(F32)
        for k in range(1, TENSOR):
            total = total + buffer[k].astype(F32)
        return total

    projected = sum_over_tensor(partial, proj1, 2, lambda: send_weights(2))
    hidden = (tokens[...].astype(F32) + projected).astype(BF16).astype(F32)

    squares = jnp.sum(hidden * hidden, axis=1, keepdims=True)
    row_of = lax.broadcasted_iota(jnp.int32, (B, HD), 0)
    lane_of = lax.broadcasted_iota(jnp.int32, (B, HD), 1)
    sq_out[...] = jnp.sum(jnp.where(row_of == lane_of, squares, 0.0), axis=0, keepdims=True)
    sq_in[rank] = sq_out[...]

    scaled = (hidden * gains[1]).astype(BF16)
    def rows_of(y2):
        return pl.ds(pl.multiple_of(y2 * ROWS_EACH, ROWS_EACH), ROWS_EACH)

    second_peers = {
        "x": [(0, dy, dz) for dy in (2, 1, 3, 0) for dz in (1, 0) if dy or dz],
        "y": [(dx, 0, dz) for dx in (2, 1, 3, 0) for dz in (1, 0) if dx or dz],
        "z": [(dx, dy, 0) for dx in (2, 1, 3, 0) for dy in (2, 1, 3, 0) if dx or dy],
    }

    def send(i, src, dst, device):
        remote(src, dst, i, device).start()

    def wait_recv(i, like):
        remote(like, like, i, peer(FAR_FIRST[-1])[1]).wait_recv()

    def wait_send(i, like):
        remote(like, like, i, peer(FAR_FIRST[-1])[1]).wait_send()

    step_0, step_1, step_2, step_3, step_4 = (7 + N_CHUNKS * i for i in range(5))
    for p, (kind, _, _) in enumerate(CHUNKS):
        wide_rows[p][:, 0:COLS] = scaled
        for offset in ring[kind]:
            to = wide_rows[p].at[:, pl.ds(step_of(offset) * COLS, COLS)]
            send(step_1 + p, wide_rows[p].at[:, pl.ds(0, COLS)], to, at(*offset)[3])
    pltpu.make_async_copy(last_weights, last_weights, own_rows_sem.at[N_CHUNKS]).wait()
    for c in range(SECTIONS):
        for half in range(2):
            product = jnp.dot(scaled, last_weights[c, half], preferred_element_type=F32)
            last_sum[c, half] = product.astype(BF16)
    for k, offset in enumerate(FAR_FIRST):
        x2, y2, z2, device = at(*offset)
        send(4, last_sum.at[x2 * NZ + z2, :, rows_of(y2)], last_in.at[k], device)
    for offset in FAR_FIRST:
        remote(sq_out, sq_in.at[rank], 3, peer(offset)[1]).start()
    row_place = {"x": dp, "y": x, "z": dp}
    for p, (kind, _, count) in enumerate(CHUNKS):
        whole = wide_weights[p].at[:, :, pl.ds(0, 128)]
        pltpu.make_async_copy(whole, whole, own_rows_sem.at[p]).wait()
        wait_recv(step_0 + p, wide_weights[p].at[:, :, pl.ds(128, 128 * (WAYS[kind] - 1))])
        wait_recv(step_1 + p, wide_rows[p].at[:, pl.ds(COLS, COLS * (WAYS[kind] - 1))])
        for i in range(NX if kind == "z" else NZ):
            for half in range(2):
                gu_sum[p][i, half] = jnp.dot(
                    wide_rows[p][...], wide_weights[p][i, half], preferred_element_type=F32
                ).astype(BF16)
        for k, offset in enumerate(second_peers[kind]):
            x2, y2, z2, device = at(*offset)
            src = gu_sum[p].at[x2 if kind == "z" else z2, :, rows_of({"x": y2, "y": x2, "z": y2}[kind])]
            send(step_2 + p, src, gu_in2[p].at[k], device)

    wait_all(sq_in.at[rest], sq_in.at[rest], 3)
    total = jnp.sum(sq_in[...], axis=0)
    lane_of = lax.broadcasted_iota(jnp.int32, (ROWS_EACH, HD), 1)
    factors = {}
    for kind in "xy":
        row_of = lax.broadcasted_iota(jnp.int32, (ROWS_EACH, HD), 0) + row_place[kind] * ROWS_EACH
        square = jnp.sum(jnp.where(row_of == lane_of, total, 0.0), axis=1, keepdims=True)
        factors[kind] = lax.rsqrt(square / D + 1e-05)
    factors["z"] = factors["x"]

    def activate_last():
        wait_recv(4, last_in)
        mine = rows_of(dp)
        halves = []
        for half in range(2):
            value = last_sum[section, half, mine].astype(F32)
            for k in range(RANKS - 1):
                value = value + last_in[k, half].astype(F32)
            halves.append(value * factors["x"])
        gate, up = halves
        last_act[section, mine] = (gate / (1.0 + jnp.exp(-gate)) * up).astype(BF16)
        block = last_act.at[section, mine]
        for offset in FAR_FIRST:
            send(5, block, block, at(*offset)[3])

    def lower_last():
        wait_recv(5, last_in.at[:, 0])
        partial = jnp.zeros((B, COLS), F32)
        for c in range(SECTIONS):
            start = c * UNITS_EACH + LAST * 128
            partial = partial + jnp.dot(
                last_act[c], down[start : start + 128], preferred_element_type=F32
            )
        lowered_sum[...] = partial

    def like_3(p):
        return gu_in2[p].at[:, 0]

    def like_4(p):
        if CHUNKS[p][0] == "z":
            return gu_sum[p].at[:, 0]
        return act[p].at[pl.ds(0, 3)]

    def activate(p):
        kind = CHUNKS[p][0]
        wait_recv(step_2 + p, gu_in2[p])
        mine = rows_of(row_place[kind])
        halves = []
        for half in range(2):
            value = gu_sum[p][x if kind == "z" else z, half, mine].astype(F32)
            for k in range(len(second_peers[kind])):
                value = value + gu_in2[p][k, half].astype(F32)
            halves.append(value * factors[kind])
        gate, up = halves
        major = dp if kind == "y" else x
        act[p][major, z, mine] = (gate / (1.0 + jnp.exp(-gate)) * up).astype(BF16)
        block = act[p].at[major, z, mine]
        for offset in second_peers[kind]:
            send(step_3 + p, block, block, at(*offset)[3])

    def pass_on(p):
        kind = CHUNKS[p][0]
        wait_recv(step_3 + p, like_3(p))
        block = {"x": act[p].at[x], "y": act[p].at[dp], "z": act[p].at[:, z]}[kind]
        for offset in ring[kind]:
            send(step_4 + p, block, block, at(*offset)[3])

    def lower(p):
        kind, first, count = CHUNKS[p]
        wait_recv(step_4 + p, like_4(p))
        width = count * 128
        partial = None
        for c in range(SECTIONS):
            start = c * UNITS_EACH + first * 128
            product = jnp.dot(
                act[p][c // NZ, c % NZ], down[start : start + width], preferred_element_type=F32
            )
            partial = product if partial is None else partial + product
        lowered_sum[...] = lowered_sum[...] + partial

    for p in range(N_CHUNKS):
        activate(p)
    activate_last()
    for p in range(N_CHUNKS):
        pass_on(p)
    loads[8].wait()
    lower_last()
    for p in range(N_CHUNKS):
        lower(p)
    partial = lowered_sum[...]
    lowered = sum_over_tensor(partial, proj2, 6)
    wait_send(4, last_in)
    wait_send(5, last_in.at[:, 0])
    for p, (kind, _, _) in enumerate(CHUNKS):
        wait_send(step_0 + p, wide_weights[p].at[:, :, pl.ds(128, 128 * (WAYS[kind] - 1))])
        wait_send(step_1 + p, wide_rows[p].at[:, pl.ds(COLS, COLS * (WAYS[kind] - 1))])
        wait_send(step_2 + p, gu_in2[p])
        wait_send(step_3 + p, like_3(p))
        wait_send(step_4 + p, like_4(p))
    out_ref[...] = hidden + lowered


def chunk_buffers():
    weights, rows, total, in2, act = [], [], [], [], []
    for kind, first, count in CHUNKS:
        w = count * 128
        blocks, peers = (NX, NX * NY - 1) if kind == "z" else (NZ, NX * NZ - 1)
        weights.append(pltpu.VMEM((blocks, 2, COLS * WAYS[kind], w), BF16))
        rows.append(pltpu.VMEM((B, COLS * WAYS[kind]), BF16))
        total.append(pltpu.VMEM((blocks, 2, B, w), BF16))
        in2.append(pltpu.VMEM((peers, 2, ROWS_EACH, w), BF16))
        act.append(pltpu.VMEM((NX, NZ, B, w), BF16))
    sums = [
        pltpu.VMEM((SECTIONS, 2, COLS, 128), BF16),
        pltpu.VMEM((SECTIONS, 2, B, 128), BF16),
        pltpu.VMEM((RANKS - 1, 2, ROWS_EACH, 128), BF16),
        pltpu.VMEM((SECTIONS, B, 128), BF16),
        pltpu.VMEM((B, COLS), F32),
        pltpu.SemaphoreType.DMA((N_CHUNKS + 1,)),
    ]
    return [*weights, *rows, *total, *in2, *act, *sums]


def body(
    tokens,
    attn_gain,
    qkv_weight,
    qkv_order,
    cache_keys,
    cache_values,
    cache_len,
    out_weight,
    ffn_gain,
    gate_up,
    down_weight,
):
    half_dim = HD // 2
    inv_freq = 500000.0 ** (-(2.0 * np.arange(half_dim)) / HD)
    inv_freq = np.concatenate([inv_freq, inv_freq])[None, :].astype(np.float32)
    hbm = pl.BlockSpec(memory_space=pl.ANY)
    out = pl.pallas_call(
        layer_kernel,
        out_shape=jax.ShapeDtypeStruct((B, COLS), F32),
        in_specs=[hbm] * 12,
        out_specs=pl.BlockSpec(memory_space=pltpu.VMEM),
        scratch_shapes=[
            pltpu.SMEM((GROUP,), jnp.int32),
            pltpu.SMEM((SEQS,), jnp.int32),
            pltpu.VMEM((1, HD), F32),
            pltpu.VMEM((B, COLS), BF16),
            pltpu.VMEM((2, 1, COLS), F32),
            pltpu.VMEM(qkv_weight.shape, BF16),
            pltpu.VMEM(cache_keys.shape, BF16),
            pltpu.VMEM(cache_values.shape, BF16),
            pltpu.VMEM(out_weight.shape, BF16),
            pltpu.VMEM(down_weight.shape, BF16),
            pltpu.VMEM((B * SLOT_ROWS, HD), F32),
            pltpu.VMEM((RANKS, SEQS * SLOT_ROWS, HD), BF16),
            pltpu.VMEM((RANKS, SEQS * SLOT_ROWS, HD), BF16),
            pltpu.VMEM((SEQS * LOCAL_HEADS, HD), F32),
            pltpu.VMEM((RANKS, SEQS * LOCAL_HEADS, HD), BF16),
            pltpu.VMEM((B * LOCAL_HEADS, HD), F32),
            pltpu.VMEM((TENSOR, B, COLS), BF16),
            pltpu.VMEM((TENSOR, B, COLS), BF16),
            pltpu.VMEM((1, 128), F32),
            pltpu.VMEM((RANKS, 1, 128), F32),
            *chunk_buffers(),
            pltpu.SemaphoreType.DMA((12,)),
            pltpu.SemaphoreType.DMA((7 + 5 * N_CHUNKS,)),
            pltpu.SemaphoreType.DMA((7 + 5 * N_CHUNKS,)),
        ],
        compiler_params=pltpu.CompilerParams(
            collective_id=0, has_side_effects=True, vmem_limit_bytes=32 * 2**20
        ),
        name="decoder_layer",
    )(
        *(
            pltpu.with_memory_space_constraint(operand, pltpu.HBM)
            for operand in (
                qkv_order,
                cache_len,
                jnp.asarray(inv_freq),
                tokens,
                attn_gain.reshape(1, COLS),
                ffn_gain.reshape(1, COLS),
                qkv_weight,
                cache_keys,
                cache_values,
                out_weight,
                gate_up,
                down_weight,
            )
        )
    )
    return out.astype(BF16)


def solution(mesh):
    rows = P(None, ("section", "dp"))
    return jax.shard_map(
        body,
        mesh=mesh,
        in_specs=(
            rows,
            P(("section", "dp")),
            P(("section", "dp"), "tensor"),
            P(),
            P(("section", "dp"), "tensor", None, None),
            P(("section", "dp"), "tensor", None, None),
            P(("section", "dp")),
            P("tensor", ("section", "dp")),
            P(("section", "dp")),
            P(None, ("section", "dp"), "tensor"),
            P("tensor", ("section", "dp")),
        ),
        out_specs=rows,
        check_vma=False,
    )
```
